1024 devices in a mesh: segment: 2 (over y_hi), win: 32 (over z), seq: 16 (over y_lo, x, core).
Axes of the slice: x: 4, y: 4 (y_hi: 2, y_lo: 2; y = y_hi * 2 + y_lo), z: 32, core: 2. Of those that a mesh axis runs over, the one named last changes fastest.
Arguments:
- latents: bfloat16 [2, 32, 1024, 1536], P('segment', 'seq', 'win'), may hold values from -6 to 6
- timesteps: int32 [2], P('segment'), may hold values from 0 to 31, as said below
- offsets: int32 [2, 2], P('segment'), may hold values from 1 to 31
- qkv_weight: bfloat16 [2, 1536, 16, 288], P('segment', None, 'seq'), may hold values from -0.15309311 to 0.15309311
- logit_scale: float32 [2, 16], P('segment', 'seq'), may hold values from 4 to 256
- out_weight: bfloat16 [2, 1536, 1536], P('segment'), may hold values from -0.15625 to 0.15625
- mod_shift: float32 [2, 32, 1536], P('segment'), may hold values from -3 to 3
- mod_scale: float32 [2, 32, 1536], P('segment'), may hold values from 0.5 to 1.5
- mod_gate: float32 [2, 32, 1536], P('segment'), may hold values from 1 to 3
Outputs:
- handed: bfloat16 [2, 32, 1024, 1536], P('segment', 'seq', 'win')
The draws below stay inside these ranges and needn't reach their ends.
Inputs may be any that keep to these rules, and one draw needn't show every extreme that they name: `timesteps`: the sections' noise levels differ from one another.
All inputs are finite; a program needn't handle non-finite values.
Results may differ from the reference program's by a relative error of at most 0.015.
Values may be sent and summed in bfloat16 or wider, within the bound.
A program may use at most 32 MiB of HBM per device.

```python
import jax
import jax.numpy as jnp
from jax import lax

D = 1536
HEADS = 16
HD = 96
WS = 32
STEPS = 32
SECTIONS = 2
HEAD_DEV = 1
LON = 1024
N_SEQ = 16


def draw_timesteps(key, part):
    order = jax.random.permutation(jax.random.fold_in(key, 29), STEPS)
    return order[:SECTIONS].astype(jnp.int32)


def draw_logit_scale(key, part):
    lows = jnp.exp(jax.random.uniform(jax.random.fold_in(key, 11), (SECTIONS, HEADS), jnp.float32, jnp.log(4.0), jnp.log(24.0)))
    return lows


def draw_qkv_weight(key, part):
    shape = (SECTIONS, D, HEADS, 3 * HD)
    spread = D ** (-0.5)
    normal = jax.random.normal(jax.random.fold_in(key, 17), shape, jnp.float32) * spread
    return jnp.clip(normal, -6.0 * spread, 6.0 * spread).astype(jnp.bfloat16)


def draw_latents(key, part):
    shape = (SECTIONS, WS, LON, D)
    return jnp.clip(jax.random.normal(jax.random.fold_in(key, 19), shape, jnp.float32), -6.0, 6.0).astype(jnp.bfloat16)


def place_ends(entries, rng, smallest, high):
    dims = entries.shape
    spot = [jax.random.randint(jax.random.fold_in(rng, axis), (), 0, dims[axis]) for axis in range(len(dims))]
    entries = entries.at[tuple(spot)].set(smallest)
    longest = dims.index(max(dims))
    spot[longest] = (spot[longest] + 1) % dims[longest]
    return entries.at[tuple(spot)].set(high)


def block_scale(own_key, dims, cuts, low, top_value):
    def one(axis_at, blocks):
        heights = jax.random.uniform(jax.random.fold_in(jax.random.fold_in(own_key, 6), axis_at), (blocks,), jnp.float32, low / len(cuts), top_value / len(cuts))
        return jnp.repeat(jnp.exp(heights), dims[axis_at] // blocks).reshape((-1,) + (1,) * (len(dims) - axis_at - 1))

    level = one(*cuts[0])
    for cut in cuts[1:]:
        level = level * one(*cut)
    return level


def bell_draw(key, extent, scale, bound, shards=(), kind=jnp.bfloat16):
    gain = block_scale(key, extent, shards, -0.22, 0.18) if shards else 1.0
    drawn = jax.random.normal(key, extent, jnp.float32) * scale * gain
    return jnp.minimum(jnp.maximum(drawn, -bound), bound).astype(kind)


def setup_inputs(seed: int = 0) -> dict:
    arg_keys = jax.random.split(jax.random.key(seed), 10)
    latents = draw_latents(jax.random.fold_in(arg_keys[9], 71), 0)
    timesteps = draw_timesteps(jax.random.fold_in(arg_keys[9], 71), 0)
    offsets = place_ends(jax.random.randint(arg_keys[2], (SECTIONS, 2), 1, WS), jax.random.fold_in(arg_keys[2], 1), 1, WS - 1).astype(jnp.int32)
    qkv_weight = draw_qkv_weight(jax.random.fold_in(arg_keys[9], 71), 0)
    logit_scale = draw_logit_scale(jax.random.fold_in(arg_keys[9], 71), 0)
    out_weight = bell_draw(arg_keys[5], (SECTIONS, HEADS * HD, D), (HEADS * HD) ** -0.5, 0.15625, ((0, 2),))
    mod_shift = bell_draw(arg_keys[6], (SECTIONS, STEPS, D), 0.5, 3.0, ((0, 2),), jnp.float32)
    mod_scale = jnp.clip(1.0 + 0.1 * jax.random.normal(arg_keys[7], (SECTIONS, STEPS, D), jnp.float32), 0.5, 1.5)
    mod_gate = jnp.clip(1.0 + 2.0 * jax.random.uniform(arg_keys[8], (SECTIONS, STEPS, D), jnp.float32) ** block_scale(arg_keys[8], (SECTIONS, STEPS, D), ((0, 2),), -0.2, 0.2), 1.0, 3.0)
    return dict(latents=latents, timesteps=timesteps, offsets=offsets, qkv_weight=qkv_weight, logit_scale=logit_scale, out_weight=out_weight, mod_shift=mod_shift, mod_scale=mod_scale, mod_gate=mod_gate)


eps_norm = 1e-06
masked = -1e+30

def unit_split(mixture, size):
    queries = mixture[..., :size]
    key_part = mixture[..., size:2 * size]
    values = mixture[..., 2 * size:]
    queries = queries * lax.rsqrt(lax.optimization_barrier(jnp.sum(queries * queries, -1, keepdims=True)) + eps_norm)
    key_part = key_part * lax.rsqrt(lax.optimization_barrier(jnp.sum(key_part * key_part, -1, keepdims=True)) + eps_norm)
    return jnp.concatenate([queries, key_part, values], -1).astype(jnp.bfloat16)

def table_row(table, noise_level):
    onehot = (jnp.arange(STEPS, dtype=jnp.int32) == noise_level).astype(jnp.float32)
    return jnp.dot(onehot, table, precision=lax.Precision.HIGHEST, preferred_element_type=jnp.float32)

def reference(latents, timesteps, offsets, qkv_weight, logit_scale, out_weight, mod_shift, mod_scale, mod_gate):
    results = []
    for section in range(SECTIONS):
        shift_row = table_row(mod_shift[section], timesteps[section])
        scale_row = table_row(mod_scale[section], timesteps[section])
        gate_row = table_row(mod_gate[section], timesteps[section])
        lat_offset = offsets[section, 0]
        lon_offset = offsets[section, 1]
        rolled = jnp.roll(latents[section], (-lat_offset, -lon_offset), axis=(0, 1))
        residual = rolled.astype(jnp.float32)
        average = lax.optimization_barrier(jnp.mean(residual, -1, keepdims=True))
        centred = residual - average
        variance = lax.optimization_barrier(jnp.mean(centred * centred, -1, keepdims=True))
        normed = (centred * lax.rsqrt(variance + eps_norm) * scale_row + shift_row).astype(jnp.bfloat16)
        windows = normed.reshape(WS, LON // WS, WS, D).transpose(1, 0, 2, 3)
        token_group = jnp.arange(WS * WS, dtype=jnp.int32) // WS >= WS - lat_offset
        allowed = token_group[:, None] == token_group[None, :]
        weights = qkv_weight[section].reshape(D, HEADS * 3 * HD)
        scales = logit_scale[section]
        grouped_out = out_weight[section].reshape(N_SEQ, HEAD_DEV * HD, D).astype(jnp.float32)

        def window_attend(window_tokens):
            flattened = window_tokens.reshape(WS * WS, D)
            mixture = jnp.dot(flattened, weights, preferred_element_type=jnp.float32).reshape(WS * WS, HEADS, 3 * HD)
            unit_heads = unit_split(mixture, HD).astype(jnp.float32)
            query_unit = unit_heads[..., :HD]
            key_unit = unit_heads[..., HD:2 * HD]
            value_rows = unit_heads[..., 2 * HD:]
            scores = jnp.einsum('qhd,khd->hqk', query_unit, key_unit, precision=lax.Precision.HIGHEST) * scales[:, None, None]
            scores = jnp.where(allowed[None], scores, masked)
            row_max = lax.optimization_barrier(jnp.max(scores, -1, keepdims=True))
            lifted = jnp.exp(scores - row_max)
            probabilities = (lifted / lax.optimization_barrier(jnp.sum(lifted, -1, keepdims=True))).astype(jnp.bfloat16)
            heads_out = jnp.einsum('hqk,khd->qhd', probabilities.astype(jnp.float32), value_rows, precision=lax.Precision.HIGHEST).astype(jnp.bfloat16)
            grouped = heads_out.reshape(WS * WS, N_SEQ, HEAD_DEV * HD).astype(jnp.float32)
            partial_value = jnp.einsum('tgk,gke->tge', grouped, grouped_out, precision=lax.Precision.HIGHEST).astype(jnp.bfloat16)
            return lax.optimization_barrier(jnp.sum(partial_value.astype(jnp.float32), 1)).astype(jnp.bfloat16).reshape(WS, WS, D)
        attention = lax.map(window_attend, windows)
        attention = attention.transpose(1, 0, 2, 3).reshape(WS, LON, D)
        updated = (residual + gate_row * attention.astype(jnp.float32)).astype(jnp.bfloat16)
        results.append(jnp.roll(updated, (lat_offset, lon_offset), axis=(0, 1)))
    stacked = jnp.stack(results)
    return jnp.roll(stacked, 1, axis=0)
```

```python
import functools
import math

import jax
import jax.numpy as jnp
from jax import lax
from jax.experimental import pallas as pl
from jax.experimental.pallas import tpu as pltpu
from jax.sharding import PartitionSpec as P

eps_norm = 1e-06
far_apart = 32768.0
LANES = 128
X_CHIPS = 4
Y_CHIPS = 2
MESH = pl.DeviceIdType.MESH

GROUPS = ((0, 0), (3, 0), (1, 0), (0, 1), (2, 0), (3, 1), (1, 1), (2, 1))


def slot_of(dx, dy, dc):
    return 2 * GROUPS.index((dx % X_CHIPS, dy % Y_CHIPS)) + dc % 2


def back_slot(slot):
    dx, dy = GROUPS[slot // 2]
    return slot_of(-dx, -dy, slot % 2)


def fused(
    wins, chunks,
    tile_ref, level_ref, offset_ref, qkv_ref, scale_ref, out_w_ref, shift_tab, scale_tab, gate_tab,
    out_ref,
    own, beside, tabs, wqkv, wout, tokens, query, key, value, heads, spread, zsend, zrecv, ysend,
    local_sem, in_sem, in_recv, send_sem, recv_sem, head_sem, head_recv, z_sem, z_recv, y_sem, y_recv,
):
    me = lax.axis_index("seq")
    win = lax.axis_index("win")
    segment = lax.axis_index("segment")
    core = lax.rem(me, 2)
    x = lax.rem(me // 2, X_CHIPS)
    y = me // (2 * X_CHIPS)

    def seq_of(slot):
        dx, dy = GROUPS[slot // 2]
        chip = lax.rem(y + dy, Y_CHIPS) * X_CHIPS + lax.rem(x + dx, X_CHIPS)
        return 2 * chip + lax.rem(core + slot % 2, 2)

    def on_seq(slot):
        return {"seq": seq_of(slot)}

    after = {"win": lax.rem(win + 1, wins)}
    before = {"win": lax.rem(win + wins - 1, wins)}
    other = {"segment": 1 - segment}
    right, left, partner, mate = slot_of(1, 0, 0), slot_of(3, 0, 0), slot_of(0, 1, 0), slot_of(0, 0, 1)

    width = own.shape[1]
    half = own.shape[0] // 2
    per_head = wout.shape[1] * 3 // 4
    count = tokens.shape[0]
    rows_in = tokens.shape[1]

    copies = [pltpu.make_async_copy(tile_ref, own, local_sem.at[0])]
    for i, tab in enumerate((shift_tab, scale_tab, gate_tab)):
        copies.append(pltpu.make_async_copy(tab, tabs.at[i], local_sem.at[1 + i]))
    for i in range(3):
        copies.append(
            pltpu.make_async_copy(
                qkv_ref.at[pl.ds(i * per_head, per_head)],
                wqkv.at[pl.ds(i * LANES, per_head)],
                local_sem.at[4 + i],
            )
        )
    for copy in copies:
        copy.start()
    out_copies = []
    for slot in range(count):
        first = pl.multiple_of(seq_of(slot) * per_head, per_head)
        copy = pltpu.make_async_copy(
            out_w_ref.at[pl.ds(first, per_head)],
            wout.at[slot, pl.ds(0, per_head)],
            local_sem.at[7 + slot],
        )
        copy.start()
        out_copies.append(copy)

    barrier = pltpu.get_barrier_semaphore()
    greeted = [after, before, other] + [on_seq(s) for s in (right, left, partner, mate)]
    for device in greeted:
        pl.semaphore_signal(barrier, inc=1, device_id=device, device_id_type=MESH)
    pl.semaphore_wait(barrier, len(greeted))

    sent = []

    def push(src, dst, send, recv, device):
        copy = pltpu.make_async_remote_copy(
            src_ref=src, dst_ref=dst, send_sem=send, recv_sem=recv, device_id=device, device_id_type=MESH
        )
        copy.start()
        sent.append(copy)

    def arrived(ref, sem):
        pltpu.make_async_remote_copy(
            src_ref=ref, dst_ref=ref, send_sem=send_sem.at[0], recv_sem=sem, device_id=after, device_id_type=MESH
        ).wait_recv()

    copies[0].wait()
    for h in range(2):
        part = pl.ds(h * half, half)
        push(own.at[part], beside.at[part], in_sem.at[h], in_recv.at[h], before)

    for i in range(3):
        wqkv[pl.ds(i * LANES + per_head, LANES - per_head), :] = jnp.zeros((LANES - per_head, width), wqkv.dtype)
    for slot in range(count):
        wout[slot, pl.ds(per_head, LANES - per_head), :] = jnp.zeros((LANES - per_head, width), wout.dtype)
    level = level_ref[0]
    lat_offset = offset_ref[0, 0]
    lon_offset = offset_ref[0, 1]
    for i in range(3):
        copies[1 + i].wait()
    shift_row = tabs[0, pl.ds(level, 1), :]
    scale_row = tabs[1, pl.ds(level, 1), :]
    gate_row = tabs[2, pl.ds(level, 1), :]
    kept = lax.broadcasted_iota(jnp.int32, (half, 1), 0) >= lon_offset

    counter = [0]

    def send_block(src_slot, h, device_slot, dst_slot):
        part = pl.ds(h * half, half)
        push(
            tokens.at[src_slot, part], tokens.at[dst_slot, part],
            send_sem.at[counter[0]], recv_sem.at[dst_slot, h], on_seq(device_slot),
        )
        counter[0] += 1

    for h in range(2):
        part = pl.ds(h * half, half)
        arrived(beside.at[part], in_recv.at[h])
        rows = jnp.where(kept, own[part, :].astype(jnp.float32), beside[part, :].astype(jnp.float32))
        centred = rows - jnp.mean(rows, -1, keepdims=True)
        variance = jnp.mean(centred * centred, -1, keepdims=True)
        normed = centred * lax.rsqrt(variance + eps_norm) * scale_row + shift_row
        tokens[0, part, :] = normed.astype(tokens.dtype)
        send_block(0, h, right, left)
        send_block(0, h, left, right)
        send_block(0, h, partner, partner)
        send_block(0, h, mate, mate)

    def take(slot, h):
        arrived(tokens.at[slot, pl.ds(h * half, half)], recv_sem.at[slot, h])

    def take_and_share(slot, h):
        take(slot, h)
        send_block(slot, h, mate, slot + 1)

    lane = lax.broadcasted_iota(jnp.int32, (2 * rows_in, LANES), 1)
    index = lax.broadcasted_iota(jnp.int32, (2 * rows_in, LANES), 0)
    second = (index // rows_in).astype(jnp.int32)
    parity = lax.rem(index // half, 2)

    def project(g):
        for h in range(2):
            take(2 * g + 1, h)
        block = tokens[pl.ds(2 * g, 2)].reshape(2 * rows_in, width)
        mixed = lax.dot_general(
            block, wqkv[...], (((1,), (1,)), ((), ())), preferred_element_type=jnp.float32
        )
        q = mixed[:, :LANES]
        k = mixed[:, LANES : 2 * LANES]
        v = mixed[:, 2 * LANES :]
        q = q * lax.rsqrt(jnp.sum(q * q, -1, keepdims=True) + eps_norm)
        k = k * lax.rsqrt(jnp.sum(k * k, -1, keepdims=True) + eps_norm)
        owner = jnp.where(second == 0, seq_of(2 * g), seq_of(2 * g + 1))
        late = 2 * owner + parity >= lat_offset
        q = jnp.where(lane == per_head, jnp.where(late, 1.0, 0.0), q)
        q = jnp.where(lane == per_head + 1, jnp.where(late, 0.0, 1.0), q)
        k = jnp.where(lane == per_head, jnp.where(late, 0.0, -far_apart), k)
        k = jnp.where(lane == per_head + 1, jnp.where(late, -far_apart, 0.0), k)
        v = jnp.where(lane == per_head, 1.0, v)
        at = pl.ds(g * 2 * rows_in, 2 * rows_in)
        query[at, :] = q.astype(query.dtype)
        key[at, :] = k.astype(key.dtype)
        value[at, :] = v.astype(value.dtype)

    far, partner_left, partner_right, partner_far = slot_of(2, 0, 0), slot_of(3, 1, 0), slot_of(1, 1, 0), slot_of(2, 1, 0)

    for i in range(3):
        copies[4 + i].wait()
    project(0)
    take_and_share(left, 0)
    send_block(left, 0, right, far)
    take_and_share(partner, 0)
    send_block(partner, 0, right, partner_left)
    send_block(partner, 0, left, partner_right)
    take_and_share(right, 0)
    take_and_share(right, 1)
    send_block(right, 1, left, far)
    take_and_share(partner, 1)
    send_block(partner, 1, right, partner_left)
    send_block(partner, 1, left, partner_right)
    take_and_share(left, 1)
    project(1)
    take_and_share(far, 0)
    send_block(far, 0, partner, partner_far)
    project(2)
    take_and_share(far, 1)
    send_block(far, 1, partner, partner_far)
    take_and_share(partner_right, 0)
    project(3)
    take_and_share(partner_left, 0)
    project(4)
    take_and_share(partner_far, 0)
    take_and_share(partner_left, 1)
    take_and_share(partner_right, 1)
    take_and_share(partner_far, 1)
    project(5)
    project(6)
    project(7)

    factor = scale_ref[0, 0] * math.log2(math.e)
    for g in reversed(range(len(GROUPS))):
        scores = lax.dot_general(
            query[pl.ds(g * 2 * rows_in, 2 * rows_in), :], key[...], (((1,), (1,)), ((), ())),
            preferred_element_type=jnp.float32,
        )
        lifted = jnp.exp2((scores - jnp.max(scores, -1, keepdims=True)) * factor)
        mixed = jnp.dot(lifted.astype(jnp.bfloat16), value[...], preferred_element_type=jnp.float32)
        mixed = mixed / mixed[:, per_head : per_head + 1]
        heads[pl.ds(2 * g, 2)] = mixed.astype(heads.dtype).reshape(2, rows_in, LANES)
        for slot in (2 * g, 2 * g + 1):
            if slot:
                to = back_slot(slot)
                push(heads.at[slot], spread.at[to], head_sem.at[slot], head_recv.at[to], on_seq(slot))
    spread[0] = heads[0]

    for copy in out_copies:
        copy.wait()
    for slot in range(1, count):
        arrived(spread.at[slot], head_recv.at[slot])
    gathered = jnp.concatenate([spread[slot] for slot in range(count)], axis=-1)
    piece = width // chunks
    for n in range(chunks):
        columns = pl.ds(n * piece, piece)
        attention = jnp.dot(
            gathered, wout[:, :, columns].reshape(count * LANES, piece), preferred_element_type=jnp.float32
        )
        zsend[n] = attention.astype(zsend.dtype)
        push(zsend.at[n], zrecv.at[n], z_sem.at[n], z_recv.at[n], after)
    column = lax.broadcasted_iota(jnp.int32, (2 * half, 1), 0)
    kept = jnp.where(column >= half, column - half, column) >= lon_offset
    for n in range(chunks):
        columns = pl.ds(n * piece, piece)
        arrived(zrecv.at[n], z_recv.at[n])
        attention = jnp.where(kept, zsend[n].astype(jnp.float32), zrecv[n].astype(jnp.float32))
        finished = own[:, columns].astype(jnp.float32) + gate_row[:, n * piece : (n + 1) * piece] * attention
        ysend[n] = finished.astype(ysend.dtype)
        push(ysend.at[n], out_ref.at[:, columns], y_sem.at[n], y_recv.at[n], other)
    for n in range(chunks):
        arrived(out_ref.at[:, pl.ds(n * piece, piece)], y_recv.at[n])
    for copy in sent:
        copy.wait_send()


def shards(
    latents, timesteps, offsets, qkv_weight, logit_scale, out_weight, mod_shift, mod_scale, mod_gate
):
    _, row_count, col_count, width = latents.shape
    head_size = qkv_weight.shape[3] // 3
    wins, seq = lax.axis_size("win"), lax.axis_size("seq")
    here = row_count * col_count
    steps = mod_shift.shape[1]
    chunks = 4 if width % 512 == 0 else 2
    piece = width // chunks
    bf16 = jnp.bfloat16
    any_space = pl.BlockSpec(memory_space=pl.ANY)
    scalars = pl.BlockSpec(memory_space=pltpu.SMEM)
    dma = pltpu.SemaphoreType.DMA
    result = pl.pallas_call(
        functools.partial(fused, wins, chunks),
        out_shape=jax.ShapeDtypeStruct((here, width), bf16),
        in_specs=[any_space, scalars, scalars, any_space, scalars] + [any_space] * 4,
        out_specs=any_space,
        scratch_shapes=[
            pltpu.VMEM((here, width), bf16),
            pltpu.VMEM((here, width), bf16),
            pltpu.VMEM((3, steps, width), jnp.float32),
            pltpu.VMEM((3 * LANES, width), bf16),
            pltpu.VMEM((seq, LANES, width), bf16),
            pltpu.VMEM((seq, here, width), bf16),
            pltpu.VMEM((seq * here, LANES), bf16),
            pltpu.VMEM((seq * here, LANES), bf16),
            pltpu.VMEM((seq * here, LANES), bf16),
            pltpu.VMEM((seq, here, LANES), bf16),
            pltpu.VMEM((seq, here, LANES), bf16),
            pltpu.VMEM((chunks, here, piece), bf16),
            pltpu.VMEM((chunks, here, piece), bf16),
            pltpu.VMEM((chunks, here, piece), bf16),
            dma((7 + seq,)),
            dma((2,)),
            dma((2,)),
            dma((32,)),
            dma((seq, 2)),
            dma((seq,)),
            dma((seq,)),
            dma((chunks,)),
            dma((chunks,)),
            dma((chunks,)),
            dma((chunks,)),
        ],
        compiler_params=pltpu.CompilerParams(
            collective_id=0, has_side_effects=True, vmem_limit_bytes=60 * 1024 * 1024
        ),
    )(
        latents.reshape(here, width),
        timesteps,
        offsets,
        qkv_weight[0, :, 0, :].T,
        logit_scale,
        out_weight[0],
        mod_shift[0],
        mod_scale[0],
        mod_gate[0],
    )
    return result.reshape(1, row_count, col_count, width)


def solution(mesh):
    in_specs = (
        P("segment", "seq", "win", None),
        P("segment"),
        P("segment", None),
        P("segment", None, "seq", None),
        P("segment", "seq"),
        P("segment", None, None),
        P("segment", None, None),
        P("segment", None, None),
        P("segment", None, None),
    )
    out_specs = P("segment", "seq", "win", None)
    return jax.shard_map(shards, mesh=mesh, in_specs=in_specs, out_specs=out_specs, check_vma=False)
```

```python
import functools
import math

import jax
import jax.numpy as jnp
from jax import lax
from jax.experimental import pallas as pl
from jax.experimental.pallas import tpu as pltpu
from jax.sharding import PartitionSpec as P

eps_norm = 1e-06
far_apart = 32768.0
LANES = 128
X_CHIPS = 4
Y_CHIPS = 2
PIECES = 4
EARLY = 10
MESH = pl.DeviceIdType.MESH

GROUPS = ((0, 0), (3, 0), (1, 0), (0, 1), (2, 0), (3, 1), (1, 1), (2, 1))


def slot_of(dx, dy, dc):
    return 2 * GROUPS.index((dx % X_CHIPS, dy % Y_CHIPS)) + dc % 2


def back_slot(slot):
    dx, dy = GROUPS[slot // 2]
    return slot_of(-dx, -dy, slot % 2)


def fused(
    wins, chunks,
    tile_ref, level_hbm, offset_hbm, qkv_ref, scale_hbm, out_w_ref, shift_tab, scale_tab, gate_tab,
    out_ref,
    level_ref, offset_ref, scale_ref,
    own, beside, tabs, wqkv, wmix, wout, tokens, late_tokens, query, key, value, heads, spread, mine, zsend, zrecv, ysend,
    local_sem, in_sem, in_recv, send_sem, recv_sem, head_sem, head_recv, z_sem, z_recv, y_sem, y_recv,
):
    me = lax.axis_index("seq")
    win = lax.axis_index("win")
    segment = lax.axis_index("segment")
    core = lax.rem(me, 2)
    x = lax.rem(me // 2, X_CHIPS)
    y = me // (2 * X_CHIPS)

    def seq_of(slot):
        dx, dy = GROUPS[slot // 2]
        chip = lax.rem(y + dy, Y_CHIPS) * X_CHIPS + lax.rem(x + dx, X_CHIPS)
        return 2 * chip + lax.rem(core + slot % 2, 2)

    def on_seq(slot):
        return {"seq": seq_of(slot)}

    right, left, partner, mate = slot_of(1, 0, 0), slot_of(3, 0, 0), slot_of(0, 1, 0), slot_of(0, 0, 1)
    far, partner_left, partner_right, partner_far = slot_of(2, 0, 0), slot_of(3, 1, 0), slot_of(1, 1, 0), slot_of(2, 1, 0)
    after = {"win": lax.rem(win + 1, wins)}
    before = {"win": lax.rem(win + wins - 1, wins)}
    other = {"segment": 1 - segment}
    across = {"segment": 1 - segment, "seq": seq_of(partner)}

    width = own.shape[1]
    here = own.shape[0]
    half = here // 2
    low = half // 2
    unit = here // PIECES
    per_head = LANES * 3 // 4
    count = spread.shape[0]

    copies = [pltpu.make_async_copy(tile_ref, own, local_sem.at[0])]
    for i, tab in enumerate((shift_tab, scale_tab, gate_tab)):
        copies.append(pltpu.make_async_copy(tab, tabs.at[i], local_sem.at[1 + i]))
    for i in range(3):
        copies.append(
            pltpu.make_async_copy(
                qkv_ref.at[pl.ds(i * per_head, per_head)],
                wqkv.at[pl.ds(i * LANES, per_head)],
                local_sem.at[4 + i],
            )
        )
    copies.append(pltpu.make_async_copy(level_hbm, level_ref, local_sem.at[7]))
    copies.append(pltpu.make_async_copy(offset_hbm, offset_ref, local_sem.at[8]))
    copies.append(pltpu.make_async_copy(scale_hbm, scale_ref, local_sem.at[9]))
    for copy in copies:
        copy.start()

    barrier = pltpu.get_barrier_semaphore()
    greeted = [after, before, across] + [on_seq(s) for s in (right, left, partner, mate)]
    for device in greeted:
        pl.semaphore_signal(barrier, inc=1, device_id=device, device_id_type=MESH)

    out_copies = []
    for slot in range(count):
        first = pl.multiple_of(seq_of(slot) * per_head, per_head)
        copy = pltpu.make_async_copy(
            out_w_ref.at[pl.ds(first, per_head)],
            wout.at[pl.ds(slot * per_head, per_head)],
            local_sem.at[10 + slot],
        )
        copy.start()
        out_copies.append(copy)
    copies[0].wait()
    pl.semaphore_wait(barrier, len(greeted))

    sent = []

    def push(src, dst, send, recv, device):
        copy = pltpu.make_async_remote_copy(
            src_ref=src, dst_ref=dst, send_sem=send, recv_sem=recv, device_id=device, device_id_type=MESH
        )
        copy.start()
        sent.append(copy)

    def arrived(ref, sem):
        pltpu.make_async_remote_copy(
            src_ref=ref, dst_ref=ref, send_sem=send_sem.at[0], recv_sem=sem, device_id=after, device_id_type=MESH
        ).wait_recv()

    sides = ((0, before), (1, after))
    for h in range(2):
        for s, device in sides:
            part = pl.ds(h * half + s * low, low)
            push(own.at[part], beside.at[part], in_sem.at[h, s], in_recv.at[h, s], device)

    for i in range(3):
        wqkv[pl.ds(i * LANES + per_head, LANES - per_head), :] = jnp.zeros((LANES - per_head, width), wqkv.dtype)
    for i in range(3):
        copies[4 + i].wait()
    wmix[...] = wqkv[...].T
    for copy in copies[7:]:
        copy.wait()
    level = level_ref[0]
    lat_offset = offset_ref[0, 0]
    lon_offset = offset_ref[0, 1]
    for i in range(3):
        copies[1 + i].wait()
    shift_row = tabs[0, pl.ds(level, 1), :]
    scale_row = tabs[1, pl.ds(level, 1), :]
    gate_row = tabs[2, pl.ds(level, 1), :]
    column = lax.broadcasted_iota(jnp.int32, (half, 1), 0)
    low_end = jnp.where(lon_offset <= low, lon_offset, 0)
    high_start = jnp.where(lon_offset <= low, half, lon_offset)

    def taken(column):
        return jnp.logical_or(column < low_end, column >= high_start)

    counter = [0]

    def piece(slot, p):
        if slot < EARLY:
            return tokens.at[slot, pl.ds(p * unit, unit)]
        return late_tokens.at[p, slot - EARLY]

    def send_piece(src_slot, p, device_slot, dst_slot):
        push(
            piece(src_slot, p), piece(dst_slot, p),
            send_sem.at[counter[0]], recv_sem.at[dst_slot, p], on_seq(device_slot),
        )
        counter[0] += 1

    for h in range(2):
        part = pl.ds(h * half, half)
        for s, _ in sides:
            arrived(beside.at[pl.ds(h * half + s * low, low)], in_recv.at[h, s])
        rows = jnp.where(taken(column), beside[part, :].astype(jnp.float32), own[part, :].astype(jnp.float32))
        centred = rows - jnp.mean(rows, -1, keepdims=True)
        variance = jnp.mean(centred * centred, -1, keepdims=True)
        normed = centred * lax.rsqrt(variance + eps_norm) * scale_row + shift_row
        tokens[0, part, :] = normed.astype(tokens.dtype)
        for p in (2 * h, 2 * h + 1):
            send_piece(0, p, partner, partner)
            if p < 3:
                send_piece(0, p, right, left)
            send_piece(0, p, left, right)
        for p in (2 * h, 2 * h + 1):
            send_piece(0, p, mate, mate)

    def take(slot, p):
        arrived(piece(slot, p), recv_sem.at[slot, p])

    def share(slot, p):
        send_piece(slot, p, mate, slot + 1)

    def project(block, owners, parities, start):
        size = block.shape[0]
        each = size // len(owners)
        mixed = jnp.dot(block, wmix[...], preferred_element_type=jnp.float32)
        q = mixed[:, :LANES]
        k = mixed[:, LANES : 2 * LANES]
        v = mixed[:, 2 * LANES :]
        q = q * lax.rsqrt(jnp.sum(q * q, -1, keepdims=True) + eps_norm)
        k = k * lax.rsqrt(jnp.sum(k * k, -1, keepdims=True) + eps_norm)
        lane = lax.broadcasted_iota(jnp.int32, (size, LANES), 1)
        index = lax.broadcasted_iota(jnp.int32, (size, LANES), 0)
        row = jnp.zeros((size, LANES), jnp.int32)
        for i, (slot, parity) in enumerate(zip(owners, parities)):
            row = jnp.where(index >= i * each, 2 * seq_of(slot) + parity, row)
        late = row >= lat_offset
        q = jnp.where(lane == per_head, jnp.where(late, 1.0, 0.0), q)
        q = jnp.where(lane == per_head + 1, jnp.where(late, 0.0, 1.0), q)
        k = jnp.where(lane == per_head, jnp.where(late, 0.0, -far_apart), k)
        k = jnp.where(lane == per_head + 1, jnp.where(late, -far_apart, 0.0), k)
        v = jnp.where(lane == per_head, 1.0, v)
        at = pl.ds(start, size)
        query[at, :] = q.astype(query.dtype)
        key[at, :] = k.astype(key.dtype)
        value[at, :] = v.astype(value.dtype)

    def project_group(g):
        for p in range(PIECES):
            take(2 * g + 1, p)
        block = tokens[pl.ds(2 * g, 2)].reshape(2 * here, width)
        project(block, (2 * g, 2 * g, 2 * g + 1, 2 * g + 1), (0, 1, 0, 1), g * 2 * here)

    late_slots = tuple(range(EARLY, count))
    late_size = len(late_slots) * unit

    def project_late(p):
        for slot in late_slots[1::2]:
            take(slot, p)
        block = late_tokens[p].reshape(late_size, width)
        project(block, late_slots, (p // 2,) * len(late_slots), EARLY * here + p * late_size)

    take(left, 0)
    send_piece(left, 0, right, far)
    send_piece(0, 3, right, left)
    share(left, 0)
    take(partner, 0)
    share(partner, 0)
    take(right, 0)
    share(right, 0)
    project_group(0)
    take(right, 1)
    send_piece(right, 1, left, far)
    share(right, 1)
    send_piece(partner, 0, left, partner_right)
    take(left, 1)
    share(left, 1)
    take(partner, 1)
    share(partner, 1)
    take(left, 2)
    send_piece(left, 2, right, far)
    share(left, 2)
    send_piece(partner, 0, right, partner_left)
    send_piece(partner, 1, right, partner_left)
    take(right, 2)
    share(right, 2)
    take(partner, 2)
    share(partner, 2)
    take(far, 0)
    send_piece(far, 0, partner, partner_far)
    share(far, 0)
    take(right, 3)
    send_piece(right, 3, left, far)
    share(right, 3)
    send_piece(partner, 1, left, partner_right)
    send_piece(partner, 2, left, partner_right)
    send_piece(partner, 2, right, partner_left)
    take(left, 3)
    share(left, 3)
    take(partner, 3)
    share(partner, 3)
    send_piece(partner, 3, right, partner_left)
    send_piece(partner, 3, left, partner_right)
    take(far, 1)
    send_piece(far, 1, partner, partner_far)
    share(far, 1)
    project_group(1)
    take(far, 2)
    send_piece(far, 2, partner, partner_far)
    share(far, 2)
    project_group(2)
    take(far, 3)
    send_piece(far, 3, partner, partner_far)
    share(far, 3)
    late_firsts = (partner_right, partner_left, partner_far)
    def take_late(p):
        for slot in late_firsts:
            take(slot, p)
            share(slot, p)

    project_group(3)
    take_late(0)
    project_group(4)
    take_late(1)
    project_late(0)
    take_late(2)
    project_late(1)
    take_late(3)
    project_late(2)
    project_late(3)

    factor = scale_ref[0, 0] * math.log2(math.e)

    def attend(start, size):
        scores = lax.dot_general(
            query[pl.ds(start, size), :], key[...], (((1,), (1,)), ((), ())), preferred_element_type=jnp.float32
        )
        lifted = jnp.exp2((scores - jnp.max(scores, -1, keepdims=True)) * factor)
        mixed = jnp.dot(lifted.astype(jnp.bfloat16), value[...], preferred_element_type=jnp.float32)
        return (mixed / mixed[:, per_head : per_head + 1]).astype(heads.dtype)

    def deliver(slot):
        if slot:
            to = back_slot(slot)
            push(heads.at[slot], spread.at[to], head_sem.at[slot], head_recv.at[to], on_seq(slot))

    mixed = attend(EARLY * here, late_size * PIECES)
    for i, slot in enumerate(late_slots):
        for p in range(PIECES):
            first = p * late_size + i * unit
            heads[slot, pl.ds(p * unit, unit), :] = mixed[first : first + unit]
    for slot in reversed(late_slots):
        deliver(slot)
    middle = 4
    for slots in (range(middle, EARLY), range(middle)):
        mixed = attend(slots[0] * here, len(slots) * here)
        heads[pl.ds(slots[0], len(slots))] = mixed.reshape(len(slots), here, LANES)
        for slot in reversed(slots):
            deliver(slot)
    spread[0] = heads[0]

    for copy in out_copies:
        copy.wait()
    for slot in range(1, count):
        arrived(spread.at[slot], head_recv.at[slot])
    gathered = jnp.concatenate([spread[slot][:, :per_head] for slot in range(count)], axis=-1)
    span = width // chunks
    for n in range(chunks):
        columns = pl.ds(n * span, span)
        attention = jnp.dot(
            gathered, wout[:, columns], preferred_element_type=jnp.float32
        ).astype(mine.dtype)
        mine[n] = attention
        for s, device in ((0, after), (1, before)):
            first = s * low
            zsend[n, s] = jnp.concatenate([attention[first : first + low], attention[half + first : half + first + low]])
            push(zsend.at[n, s], zrecv.at[n, s], z_sem.at[n, s], z_recv.at[n, s], device)
    column = lax.broadcasted_iota(jnp.int32, (here, 1), 0)
    given = taken(jnp.where(column >= half, column - half, column))
    for n in range(chunks):
        columns = pl.ds(n * span, span)
        for s, _ in sides:
            arrived(zrecv.at[n, s], z_recv.at[n, s])
        lows, highs = zrecv[n, 0], zrecv[n, 1]
        theirs = jnp.concatenate([lows[:low], highs[:low], lows[low:], highs[low:]])
        attention = jnp.where(given, theirs.astype(jnp.float32), mine[n].astype(jnp.float32))
        finished = own[:, columns].astype(jnp.float32) + gate_row[:, n * span : (n + 1) * span] * attention
        ysend[n] = finished.astype(ysend.dtype)
        push(ysend.at[n], out_ref.at[:, columns], y_sem.at[n], y_recv.at[n], other)
    for n in range(chunks):
        arrived(out_ref.at[:, pl.ds(n * span, span)], y_recv.at[n])
    for copy in sent:
        copy.wait_send()


def shards(
    latents, timesteps, offsets, qkv_weight, logit_scale, out_weight, mod_shift, mod_scale, mod_gate
):
    _, row_count, col_count, width = latents.shape
    wins, seq = lax.axis_size("win"), lax.axis_size("seq")
    here = row_count * col_count
    unit = here // PIECES
    steps = mod_shift.shape[1]
    chunks = 3 if width % 384 == 0 else 2
    span = width // chunks
    bf16 = jnp.bfloat16
    in_hbm = pl.BlockSpec(memory_space=pltpu.HBM)
    dma = pltpu.SemaphoreType.DMA
    result = pl.pallas_call(
        functools.partial(fused, wins, chunks),
        out_shape=pltpu.VMEM((here, width), bf16),
        in_specs=[in_hbm] * 9,
        out_specs=pl.BlockSpec(memory_space=pltpu.VMEM),
        scratch_shapes=[
            pltpu.SMEM((1,), jnp.int32),
            pltpu.SMEM((1, 2), jnp.int32),
            pltpu.SMEM((1, 1), jnp.float32),
            pltpu.VMEM((here, width), bf16),
            pltpu.VMEM((here, width), bf16),
            pltpu.VMEM((3, steps, width), jnp.float32),
            pltpu.VMEM((3 * LANES, width), bf16),
            pltpu.VMEM((width, 3 * LANES), bf16),
            pltpu.VMEM((seq * (LANES * 3 // 4), width), bf16),
            pltpu.VMEM((EARLY, here, width), bf16),
            pltpu.VMEM((PIECES, seq - EARLY, unit, width), bf16),
            pltpu.VMEM((seq * here, LANES), bf16),
            pltpu.VMEM((seq * here, LANES), bf16),
            pltpu.VMEM((seq * here, LANES), bf16),
            pltpu.VMEM((seq, here, LANES), bf16),
            pltpu.VMEM((seq, here, LANES), bf16),
            pltpu.VMEM((chunks, here, span), bf16),
            pltpu.VMEM((chunks, 2, here // 2, span), bf16),
            pltpu.VMEM((chunks, 2, here // 2, span), bf16),
            pltpu.VMEM((chunks, here, span), bf16),
            dma((10 + seq,)),
            dma((2, 2)),
            dma((2, 2)),
            dma((64,)),
            dma((seq, PIECES)),
            dma((seq,)),
            dma((seq,)),
            dma((chunks, 2)),
            dma((chunks, 2)),
            dma((chunks,)),
            dma((chunks,)),
        ],
        compiler_params=pltpu.CompilerParams(
            collective_id=0, has_side_effects=True, vmem_limit_bytes=56 * 1024 * 1024
        ),
    )(
        latents.reshape(here, width),
        timesteps,
        offsets,
        qkv_weight[0, :, 0, :].T,
        logit_scale,
        out_weight[0],
        mod_shift[0],
        mod_scale[0],
        mod_gate[0],
    )
    return result.reshape(1, row_count, col_count, width)


def solution(mesh):
    in_specs = (
        P("segment", "seq", "win", None),
        P("segment"),
        P("segment", None),
        P("segment", None, "seq", None),
        P("segment", "seq"),
        P("segment", None, None),
        P("segment", None, None),
        P("segment", None, None),
        P("segment", None, None),
    )
    out_specs = P("segment", "seq", "win", None)
    return jax.shard_map(shards, mesh=mesh, in_specs=in_specs, out_specs=out_specs, check_vma=False)
```

```python
import functools
import math

import jax
import jax.numpy as jnp
from jax import lax
from jax.experimental import pallas as pl
from jax.experimental.pallas import tpu as pltpu
from jax.sharding import PartitionSpec as P

eps_norm = 1e-06
far_apart = 32768.0
LANES = 128
X_CHIPS = 4
Y_CHIPS = 2
PIECES = 4
EARLY = 10
MESH = pl.DeviceIdType.MESH

GROUPS = ((0, 0), (3, 0), (1, 0), (0, 1), (2, 0), (3, 1), (1, 1), (2, 1))


def slot_of(dx, dy, dc):
    return 2 * GROUPS.index((dx % X_CHIPS, dy % Y_CHIPS)) + dc % 2


def back_slot(slot):
    dx, dy = GROUPS[slot // 2]
    return slot_of(-dx, -dy, slot % 2)


def fused(
    wins, chunks,
    tile_ref, level_hbm, offset_hbm, qkv_ref, scale_hbm, out_w_ref, shift_tab, scale_tab, gate_tab,
    out_ref,
    level_ref, offset_ref, scale_ref,
    own, beside, tabs, wqkv, wmix, wout, tokens, late_tokens, query, key, value, heads, spread, mine, theirs, ysend,
    local_sem, sent, in_recv, recv_sem, mate_recv, late_recv, head_recv, z_recv, y_recv,
):
    me = lax.axis_index("seq")
    win = lax.axis_index("win")
    segment = lax.axis_index("segment")
    core = lax.rem(me, 2)
    x = lax.rem(me // 2, X_CHIPS)
    y = me // (2 * X_CHIPS)

    def seq_of(slot):
        dx, dy = GROUPS[slot // 2]
        chip = lax.rem(y + dy, Y_CHIPS) * X_CHIPS + lax.rem(x + dx, X_CHIPS)
        return 2 * chip + lax.rem(core + slot % 2, 2)

    def on_seq(slot):
        return {"seq": seq_of(slot)}

    right, left, partner, mate = slot_of(1, 0, 0), slot_of(3, 0, 0), slot_of(0, 1, 0), slot_of(0, 0, 1)
    far, partner_left, partner_right, partner_far = slot_of(2, 0, 0), slot_of(3, 1, 0), slot_of(1, 1, 0), slot_of(2, 1, 0)
    after = {"win": lax.rem(win + 1, wins)}
    before = {"win": lax.rem(win + wins - 1, wins)}
    other = {"segment": 1 - segment}
    across = {"segment": 1 - segment, "seq": seq_of(partner)}

    width = own.shape[1]
    here = own.shape[0]
    half = here // 2
    low = half // 2
    unit = here // PIECES
    per_head = LANES * 3 // 4
    count = spread.shape[1]

    pltpu.make_async_copy(tile_ref, own, local_sem.at[0]).start()
    for i, tab in enumerate((shift_tab, scale_tab, gate_tab)):
        pltpu.make_async_copy(tab, tabs.at[i], local_sem.at[1]).start()
    for i in range(3):
        pltpu.make_async_copy(
            qkv_ref.at[pl.ds(i * per_head, per_head)], wqkv.at[pl.ds(i * LANES, per_head)], local_sem.at[2]
        ).start()
    scalars = [
        pltpu.make_async_copy(src, dst, local_sem.at[3 + i])
        for i, (src, dst) in enumerate(((level_hbm, level_ref), (offset_hbm, offset_ref), (scale_hbm, scale_ref)))
    ]
    for copy in scalars:
        copy.start()

    barrier = pltpu.get_barrier_semaphore()
    greeted = [after, before, across] + [on_seq(s) for s in (right, left, partner, mate)]
    for device in greeted:
        pl.semaphore_signal(barrier, inc=1, device_id=device, device_id_type=MESH)

    for slot in range(count):
        first = pl.multiple_of(seq_of(slot) * per_head, per_head)
        pltpu.make_async_copy(
            out_w_ref.at[pl.ds(first, per_head)], wout.at[pl.ds(slot * per_head, per_head)], local_sem.at[6]
        ).start()
    pltpu.make_async_copy(tile_ref, own, local_sem.at[0]).wait()
    pl.semaphore_wait(barrier, len(greeted))

    def push(src, dst, send, recv, device):
        pltpu.make_async_remote_copy(
            src_ref=src, dst_ref=dst, send_sem=send, recv_sem=recv, device_id=device, device_id_type=MESH
        ).start()

    def arrived(ref, sem):
        pltpu.make_async_remote_copy(
            src_ref=ref, dst_ref=ref, send_sem=sent.at[0], recv_sem=sem, device_id=after, device_id_type=MESH
        ).wait_recv()

    def left_here(ref, sem):
        pltpu.make_async_remote_copy(
            src_ref=ref, dst_ref=ref, send_sem=sem, recv_sem=in_recv.at[0], device_id=after, device_id_type=MESH
        ).wait_send()

    sides = ((0, before), (1, after))
    for h in range(2):
        for s, device in sides:
            part = pl.ds(h * half + s * low, low)
            push(own.at[part], beside.at[part], sent.at[0], in_recv.at[h], device)

    for i in range(3):
        wqkv[pl.ds(i * LANES + per_head, LANES - per_head), :] = jnp.zeros((LANES - per_head, width), wqkv.dtype)
    pltpu.make_async_copy(qkv_ref, wqkv.at[pl.ds(0, 3 * per_head)], local_sem.at[2]).wait()
    wmix[...] = wqkv[...].T
    for copy in scalars:
        copy.wait()
    level = level_ref[0]
    lat_offset = offset_ref[0, 0]
    lon_offset = offset_ref[0, 1]
    pltpu.make_async_copy(tabs, tabs, local_sem.at[1]).wait()
    shift_row = tabs[0, pl.ds(level, 1), :]
    scale_row = tabs[1, pl.ds(level, 1), :]
    gate_row = tabs[2, pl.ds(level, 1), :]
    column = lax.broadcasted_iota(jnp.int32, (half, 1), 0)
    low_end = jnp.where(lon_offset <= low, lon_offset, 0)
    high_start = jnp.where(lon_offset <= low, half, lon_offset)

    def taken(column):
        return jnp.logical_or(column < low_end, column >= high_start)

    late_slots = tuple(range(EARLY, count))
    late_count = len(late_slots) // 2
    late_size = len(late_slots) * unit
    late_order = late_slots[::2] + late_slots[1::2]
    sends = [0]

    def piece(slot, p):
        if slot < EARLY:
            return tokens.at[slot, pl.ds(p * unit, unit)]
        return late_tokens.at[p, late_order.index(slot)]

    def arrival(slot, p):
        if slot >= EARLY:
            return late_recv.at[slot % 2, p]
        return mate_recv.at[slot // 2] if slot % 2 else recv_sem.at[slot // 2, p]

    def send_piece(src_slot, p, device_slot, dst_slot):
        lot = 1 if sends[0] < EARLY * PIECES else 2
        push(piece(src_slot, p), piece(dst_slot, p), sent.at[lot], arrival(dst_slot, p), on_seq(device_slot))
        sends[0] += 1

    for h in range(2):
        part = pl.ds(h * half, half)
        arrived(beside.at[part], in_recv.at[h])
        rows = jnp.where(taken(column), beside[part, :].astype(jnp.float32), own[part, :].astype(jnp.float32))
        centred = rows - jnp.mean(rows, -1, keepdims=True)
        variance = jnp.mean(centred * centred, -1, keepdims=True)
        normed = centred * lax.rsqrt(variance + eps_norm) * scale_row + shift_row
        tokens[0, part, :] = normed.astype(tokens.dtype)
        for p in (2 * h, 2 * h + 1):
            send_piece(0, p, partner, partner)
            send_piece(0, p, right, left)
            send_piece(0, p, left, right)
        for p in (2 * h, 2 * h + 1):
            send_piece(0, p, mate, mate)

    def take(slot, p):
        arrived(piece(slot, p), arrival(slot, p))

    def share(slot, p):
        send_piece(slot, p, mate, slot + 1)

    def project(block, owners, parities, start, places):
        size = block.shape[0]
        each = size // len(owners)
        mixed = jnp.dot(block, wmix[...], preferred_element_type=jnp.float32)
        q = mixed[:, :LANES]
        k = mixed[:, LANES : 2 * LANES]
        v = mixed[:, 2 * LANES :]
        q = q * lax.rsqrt(jnp.sum(q * q, -1, keepdims=True) + eps_norm)
        k = k * lax.rsqrt(jnp.sum(k * k, -1, keepdims=True) + eps_norm)
        lane = lax.broadcasted_iota(jnp.int32, (size, LANES), 1)
        index = lax.broadcasted_iota(jnp.int32, (size, LANES), 0)
        row = jnp.zeros((size, LANES), jnp.int32)
        for i, (slot, parity) in enumerate(zip(owners, parities)):
            row = jnp.where(index >= i * each, 2 * seq_of(slot) + parity, row)
        late = row >= lat_offset
        q = jnp.where(lane == per_head, jnp.where(late, 1.0, 0.0), q)
        q = jnp.where(lane == per_head + 1, jnp.where(late, 0.0, 1.0), q)
        k = jnp.where(lane == per_head, jnp.where(late, 0.0, -far_apart), k)
        k = jnp.where(lane == per_head + 1, jnp.where(late, -far_apart, 0.0), k)
        v = jnp.where(lane == per_head, 1.0, v)
        q = q.astype(query.dtype)
        for first, h, place, extent in places:
            query[h, pl.ds(place, extent), :] = q[first : first + extent]
        at = pl.ds(start, size)
        key[at, :] = k.astype(key.dtype)
        value[at, :] = v.astype(value.dtype)

    def project_groups(g, n):
        for slot in range(2 * g + 1, 2 * (g + n), 2):
            arrived(tokens.at[slot], mate_recv.at[slot // 2])
        block = tokens[pl.ds(2 * g, 2 * n)].reshape(2 * n * here, width)
        slots = range(2 * g, 2 * (g + n))
        project(
            block, [slot for slot in slots for _ in range(2)], (0, 1) * (2 * n), g * 2 * here,
            tuple((i * half, i % 2, (2 * g + i // 2) * half, half) for i in range(4 * n)),
        )

    def project_late(p, n):
        for q in range(p, p + n):
            arrived(late_tokens.at[q, pl.ds(late_count, late_count)], late_recv.at[1, q])
        size = n * late_size
        block = late_tokens[pl.ds(p, n)].reshape(size, width)
        project(
            block, late_order * n, (p // 2,) * (n * len(late_slots)), EARLY * here + p * late_size,
            ((0, p // 2, EARLY * half + p % 2 * late_size, size),),
        )

    take(left, 0)
    send_piece(left, 0, right, far)
    send_piece(left, 0, partner, partner_left)
    share(left, 0)
    take(partner, 0)
    share(partner, 0)
    take(right, 0)
    send_piece(right, 0, partner, partner_right)
    share(right, 0)
    project_groups(0, 1)
    take(right, 1)
    send_piece(right, 1, left, far)
    share(right, 1)
    take(partner, 1)
    send_piece(partner, 1, left, partner_right)
    share(partner, 1)
    take(left, 1)
    share(left, 1)
    take(left, 2)
    send_piece(left, 2, right, far)
    send_piece(partner, 1, right, partner_left)
    share(left, 2)
    take(partner, 2)
    share(partner, 2)
    take(right, 2)
    share(right, 2)
    take(right, 3)
    send_piece(right, 3, left, far)
    share(right, 3)
    send_piece(partner, 2, left, partner_right)
    send_piece(partner, 2, right, partner_left)
    take(partner, 3)
    send_piece(partner, 3, right, partner_left)
    send_piece(partner, 3, left, partner_right)
    share(partner, 3)
    take(left, 3)
    share(left, 3)

    def take_far(p):
        take(far, p)
        send_piece(far, p, partner, partner_far)
        share(far, p)

    def take_late(p):
        mine_here = late_tokens.at[p, pl.ds(0, late_count)]
        arrived(mine_here, late_recv.at[0, p])
        push(mine_here, late_tokens.at[p, pl.ds(late_count, late_count)], sent.at[3], late_recv.at[1, p], on_seq(mate))

    take_far(0)
    project_groups(1, 1)
    take_far(1)
    take_far(2)
    project_groups(2, 2)
    take_far(3)
    take_late(0)
    project_groups(4, 1)
    take_late(1)
    take_late(2)
    take_late(3)
    project_late(0, 2)
    project_late(2, 2)

    factor = scale_ref[0, 0] * math.log2(math.e)

    def scores_of(h, start, size):
        return lax.dot_general(
            query[h, pl.ds(start, size), :], key[...], (((1,), (1,)), ((), ())), preferred_element_type=jnp.float32
        )

    def attend(scores):
        lifted = jnp.exp2((scores - jnp.max(scores, -1, keepdims=True)) * factor)
        mixed = jnp.dot(lifted.astype(jnp.bfloat16), value[...], preferred_element_type=jnp.float32)
        return (mixed / mixed[:, per_head : per_head + 1]).astype(heads.dtype)

    def deliver(slot, h):
        if slot:
            to = back_slot(slot)
            push(heads.at[h, slot], spread.at[h, to], sent.at[4], head_recv.at[h], on_seq(slot))

    middle = count // 2
    blocks = [(h, start) for h in range(2) for start in (middle, 0)]
    upcoming = scores_of(blocks[0][0], blocks[0][1] * half, middle * half)
    for i, (h, start) in enumerate(blocks):
        scores = upcoming
        if i + 1 < len(blocks):
            upcoming = scores_of(blocks[i + 1][0], blocks[i + 1][1] * half, middle * half)
        mixed = attend(scores)
        if start:
            for slot in range(middle, EARLY):
                first = (slot - middle) * half
                heads[h, slot] = mixed[first : first + half]
            for k, slot in enumerate(late_order):
                for p in range(2):
                    first = (EARLY - middle) * half + p * late_size + k * unit
                    heads[h, slot, pl.ds(p * unit, unit), :] = mixed[first : first + unit]
        else:
            heads[h, pl.ds(0, middle)] = mixed.reshape(middle, half, LANES)
            spread[h, 0] = heads[h, 0]
        for slot in reversed(range(start, start + middle)):
            deliver(slot, h)

    span = width // chunks
    pltpu.make_async_copy(out_w_ref, wout, local_sem.at[6]).wait()
    for h in range(2):
        arrived(spread.at[h, pl.ds(1, count - 1)], head_recv.at[h])
        gathered = jnp.concatenate([spread[h, slot][:, :per_head] for slot in range(count)], axis=-1)
        for n in range(chunks):
            attention = jnp.dot(gathered, wout[:, pl.ds(n * span, span)], preferred_element_type=jnp.float32)
            mine[h, n] = attention.astype(mine.dtype)
            for s, device in ((0, after), (1, before)):
                part = pl.ds(s * low, low)
                push(mine.at[h, n, part], theirs.at[h, n, part], sent.at[5], z_recv.at[h, n], device)
    for h in range(2):
        for n in range(chunks):
            rows, columns = pl.ds(h * half, half), pl.ds(n * span, span)
            arrived(theirs.at[h, n], z_recv.at[h, n])
            attention = jnp.where(taken(column), theirs[h, n].astype(jnp.float32), mine[h, n].astype(jnp.float32))
            finished = own[rows, columns].astype(jnp.float32) + gate_row[:, n * span : (n + 1) * span] * attention
            ysend[h, n] = finished.astype(ysend.dtype)
            push(ysend.at[h, n], out_ref.at[rows, columns], sent.at[6], y_recv.at[0], other)
    assert sends[0] == 12 * PIECES
    left_here(own, sent.at[0])
    left_here(tokens, sent.at[1])
    left_here(tokens.at[pl.ds(0, sends[0] // PIECES - EARLY)], sent.at[2])
    left_here(late_tokens.at[:, pl.ds(0, late_count)], sent.at[3])
    left_here(heads.at[:, pl.ds(1, count - 1)], sent.at[4])
    left_here(mine, sent.at[5])
    arrived(out_ref, y_recv.at[0])
    left_here(ysend, sent.at[6])


def shards(
    latents, timesteps, offsets, qkv_weight, logit_scale, out_weight, mod_shift, mod_scale, mod_gate
):
    _, row_count, col_count, width = latents.shape
    wins, seq = lax.axis_size("win"), lax.axis_size("seq")
    here = row_count * col_count
    half = here // 2
    unit = here // PIECES
    steps = mod_shift.shape[1]
    chunks = 3 if width % 384 == 0 else 2
    span = width // chunks
    bf16 = jnp.bfloat16
    in_hbm = pl.BlockSpec(memory_space=pltpu.HBM)
    dma = pltpu.SemaphoreType.DMA
    result = pl.pallas_call(
        functools.partial(fused, wins, chunks),
        out_shape=pltpu.VMEM((here, width), bf16),
        in_specs=[in_hbm] * 9,
        out_specs=pl.BlockSpec(memory_space=pltpu.VMEM),
        scratch_shapes=[
            pltpu.SMEM((1,), jnp.int32),
            pltpu.SMEM((1, 2), jnp.int32),
            pltpu.SMEM((1, 1), jnp.float32),
            pltpu.VMEM((here, width), bf16),
            pltpu.VMEM((here, width), bf16),
            pltpu.VMEM((3, steps, width), jnp.float32),
            pltpu.VMEM((3 * LANES, width), bf16),
            pltpu.VMEM((width, 3 * LANES), bf16),
            pltpu.VMEM((seq * (LANES * 3 // 4), width), bf16),
            pltpu.VMEM((EARLY, here, width), bf16),
            pltpu.VMEM((PIECES, seq - EARLY, unit, width), bf16),
            pltpu.VMEM((2, seq * half, LANES), bf16),
            pltpu.VMEM((seq * here, LANES), bf16),
            pltpu.VMEM((seq * here, LANES), bf16),
            pltpu.VMEM((2, seq, half, LANES), bf16),
            pltpu.VMEM((2, seq, half, LANES), bf16),
            pltpu.VMEM((2, chunks, half, span), bf16),
            pltpu.VMEM((2, chunks, half, span), bf16),
            pltpu.VMEM((2, chunks, half, span), bf16),
            dma((7,)),
            dma((7,)),
            dma((2,)),
            dma((EARLY // 2, PIECES)),
            dma((EARLY // 2,)),
            dma((2, PIECES)),
            dma((2,)),
            dma((2, chunks)),
            dma((1,)),
        ],
        compiler_params=pltpu.CompilerParams(
            collective_id=0, has_side_effects=True, vmem_limit_bytes=56 * 1024 * 1024
        ),
    )(
        latents.reshape(here, width),
        timesteps,
        offsets,
        qkv_weight[0, :, 0, :].T,
        logit_scale,
        out_weight[0],
        mod_shift[0],
        mod_scale[0],
        mod_gate[0],
    )
    return result.reshape(1, row_count, col_count, width)


def solution(mesh):
    in_specs = (
        P("segment", "seq", "win", None),
        P("segment"),
        P("segment", None),
        P("segment", None, "seq", None),
        P("segment", "seq"),
        P("segment", None, None),
        P("segment", None, None),
        P("segment", None, None),
        P("segment", None, None),
    )
    out_specs = P("segment", "seq", "win", None)
    return jax.shard_map(shards, mesh=mesh, in_specs=in_specs, out_specs=out_specs, check_vma=False)
```

```python
import functools
import math

import jax
import jax.numpy as jnp
from jax import lax
from jax.experimental import pallas as pl
from jax.experimental.pallas import tpu as pltpu
from jax.sharding import PartitionSpec as P

eps_norm = 1e-06
far_apart = 32768.0
LANES = 128
X_CHIPS = 4
Y_CHIPS = 2
PIECES = 4
EARLY = 10
MESH = pl.DeviceIdType.MESH

GROUPS = ((0, 0), (3, 0), (1, 0), (0, 1), (2, 0), (3, 1), (1, 1), (2, 1))


def slot_of(dx, dy, dc):
    return 2 * GROUPS.index((dx % X_CHIPS, dy % Y_CHIPS)) + dc % 2


def back_slot(slot):
    dx, dy = GROUPS[slot // 2]
    return slot_of(-dx, -dy, slot % 2)


def fused(
    wins, chunks,
    tile_ref, level_hbm, offset_hbm, qkv_ref, scale_hbm, out_w_ref, shift_tab, scale_tab, gate_tab,
    out_ref,
    level_ref, offset_ref, scale_ref,
    own, beside, tabs, wqkv, wmix, wout, tokens, late_tokens, query, key, value, heads, spread, mine, theirs, ysend,
    local_sem, sent, in_recv, recv_sem, mate_recv, late_recv, far_recv, head_recv, z_recv, y_recv,
):
    me = lax.axis_index("seq")
    win = lax.axis_index("win")
    segment = lax.axis_index("segment")
    core = lax.rem(me, 2)
    x = lax.rem(me // 2, X_CHIPS)
    y = me // (2 * X_CHIPS)

    def seq_of(slot):
        dx, dy = GROUPS[slot // 2]
        chip = lax.rem(y + dy, Y_CHIPS) * X_CHIPS + lax.rem(x + dx, X_CHIPS)
        return 2 * chip + lax.rem(core + slot % 2, 2)

    def on_seq(slot):
        return {"seq": seq_of(slot)}

    right, left, partner, mate = slot_of(1, 0, 0), slot_of(3, 0, 0), slot_of(0, 1, 0), slot_of(0, 0, 1)
    far, partner_left, partner_right, partner_far = slot_of(2, 0, 0), slot_of(3, 1, 0), slot_of(1, 1, 0), slot_of(2, 1, 0)
    after = {"win": lax.rem(win + 1, wins)}
    before = {"win": lax.rem(win + wins - 1, wins)}
    other = {"segment": 1 - segment}
    across = {"segment": 1 - segment, "seq": seq_of(partner)}

    width = own.shape[1]
    here = own.shape[0]
    half = here // 2
    low = half // 2
    unit = here // PIECES
    per_head = LANES * 3 // 4
    count = spread.shape[1]

    pltpu.make_async_copy(tile_ref, own, local_sem.at[0]).start()
    for i, tab in enumerate((shift_tab, scale_tab, gate_tab)):
        pltpu.make_async_copy(tab, tabs.at[i], local_sem.at[1]).start()
    for i in range(3):
        pltpu.make_async_copy(
            qkv_ref.at[pl.ds(i * per_head, per_head)], wqkv.at[pl.ds(i * LANES, per_head)], local_sem.at[2]
        ).start()
    scalars = [
        pltpu.make_async_copy(src, dst, local_sem.at[3 + i])
        for i, (src, dst) in enumerate(((level_hbm, level_ref), (offset_hbm, offset_ref), (scale_hbm, scale_ref)))
    ]
    for copy in scalars:
        copy.start()

    barrier = pltpu.get_barrier_semaphore()
    greeted = [after, before, across] + [on_seq(s) for s in (right, left, partner, mate)]
    for device in greeted:
        pl.semaphore_signal(barrier, inc=1, device_id=device, device_id_type=MESH)

    for slot in range(count):
        first = pl.multiple_of(seq_of(slot) * per_head, per_head)
        pltpu.make_async_copy(
            out_w_ref.at[pl.ds(first, per_head)], wout.at[pl.ds(slot * per_head, per_head)], local_sem.at[6]
        ).start()
    pltpu.make_async_copy(tile_ref, own, local_sem.at[0]).wait()
    pl.semaphore_wait(barrier, len(greeted))

    def push(src, dst, send, recv, device):
        pltpu.make_async_remote_copy(
            src_ref=src, dst_ref=dst, send_sem=send, recv_sem=recv, device_id=device, device_id_type=MESH
        ).start()

    def arrived(ref, sem):
        pltpu.make_async_remote_copy(
            src_ref=ref, dst_ref=ref, send_sem=sent.at[0], recv_sem=sem, device_id=after, device_id_type=MESH
        ).wait_recv()

    def left_here(ref, sem):
        pltpu.make_async_remote_copy(
            src_ref=ref, dst_ref=ref, send_sem=sem, recv_sem=in_recv.at[0], device_id=after, device_id_type=MESH
        ).wait_send()

    sides = ((0, before), (1, after))
    for h in range(2):
        for s, device in sides:
            part = pl.ds(h * half + s * low, low)
            push(own.at[part], beside.at[part], sent.at[0], in_recv.at[h], device)

    for i in range(3):
        wqkv[pl.ds(i * LANES + per_head, LANES - per_head), :] = jnp.zeros((LANES - per_head, width), wqkv.dtype)
    pltpu.make_async_copy(qkv_ref, wqkv.at[pl.ds(0, 3 * per_head)], local_sem.at[2]).wait()
    wmix[...] = wqkv[...].T
    for copy in scalars:
        copy.wait()
    level = level_ref[0]
    lat_offset = offset_ref[0, 0]
    lon_offset = offset_ref[0, 1]
    pltpu.make_async_copy(tabs, tabs, local_sem.at[1]).wait()
    shift_row = tabs[0, pl.ds(level, 1), :]
    scale_row = tabs[1, pl.ds(level, 1), :]
    gate_row = tabs[2, pl.ds(level, 1), :]
    column = lax.broadcasted_iota(jnp.int32, (half, 1), 0)
    low_end = jnp.where(lon_offset <= low, lon_offset, 0)
    high_start = jnp.where(lon_offset <= low, half, lon_offset)

    def taken(column):
        return jnp.logical_or(column < low_end, column >= high_start)

    late_slots = tuple(range(EARLY, count))
    late_count = len(late_slots) // 2
    late_size = len(late_slots) * unit
    late_order = late_slots[::2] + late_slots[1::2]
    sends = [0]

    def piece(slot, p):
        if slot < EARLY:
            return tokens.at[slot, pl.ds(p * unit, unit)]
        return late_tokens.at[p, late_order.index(slot)]

    def arrival(slot, p):
        if (slot, p) == (partner_left, 0):
            return far_recv.at[PIECES]
        if slot == partner_far:
            return far_recv.at[p]
        if slot >= EARLY:
            return late_recv.at[slot % 2, p]
        return mate_recv.at[slot // 2] if slot % 2 else recv_sem.at[slot // 2, p]

    def send_piece(src_slot, p, device_slot, dst_slot):
        lot = 1 if sends[0] < EARLY * PIECES else 2
        push(piece(src_slot, p), piece(dst_slot, p), sent.at[lot], arrival(dst_slot, p), on_seq(device_slot))
        sends[0] += 1

    for h in range(2):
        part = pl.ds(h * half, half)
        arrived(beside.at[part], in_recv.at[h])
        rows = jnp.where(taken(column), beside[part, :].astype(jnp.float32), own[part, :].astype(jnp.float32))
        centred = rows - jnp.mean(rows, -1, keepdims=True)
        variance = jnp.mean(centred * centred, -1, keepdims=True)
        normed = centred * lax.rsqrt(variance + eps_norm) * scale_row + shift_row
        tokens[0, part, :] = normed.astype(tokens.dtype)
        for p in (2 * h, 2 * h + 1):
            send_piece(0, p, partner, partner)
            send_piece(0, p, right, left)
            send_piece(0, p, left, right)
        for p in (2 * h, 2 * h + 1):
            send_piece(0, p, mate, mate)

    def take(slot, p):
        arrived(piece(slot, p), arrival(slot, p))

    def share(slot, p):
        send_piece(slot, p, mate, slot + 1)

    def project(block, owners, parities, start, places):
        size = block.shape[0]
        each = size // len(owners)
        mixed = jnp.dot(block, wmix[...], preferred_element_type=jnp.float32)
        q = mixed[:, :LANES]
        k = mixed[:, LANES : 2 * LANES]
        v = mixed[:, 2 * LANES :]
        q = q * lax.rsqrt(jnp.sum(q * q, -1, keepdims=True) + eps_norm)
        k = k * lax.rsqrt(jnp.sum(k * k, -1, keepdims=True) + eps_norm)
        lane = lax.broadcasted_iota(jnp.int32, (size, LANES), 1)
        index = lax.broadcasted_iota(jnp.int32, (size, LANES), 0)
        row = jnp.zeros((size, LANES), jnp.int32)
        for i, (slot, parity) in enumerate(zip(owners, parities)):
            row = jnp.where(index >= i * each, 2 * seq_of(slot) + parity, row)
        late = row >= lat_offset
        q = jnp.where(lane == per_head, jnp.where(late, 1.0, 0.0), q)
        q = jnp.where(lane == per_head + 1, jnp.where(late, 0.0, 1.0), q)
        k = jnp.where(lane == per_head, jnp.where(late, 0.0, -far_apart), k)
        k = jnp.where(lane == per_head + 1, jnp.where(late, -far_apart, 0.0), k)
        v = jnp.where(lane == per_head, 1.0, v)
        q = q.astype(query.dtype)
        for first, h, place, extent in places:
            query[h, pl.ds(place, extent), :] = q[first : first + extent]
        at = pl.ds(start, size)
        key[at, :] = k.astype(key.dtype)
        value[at, :] = v.astype(value.dtype)

    def project_groups(g, n):
        for slot in range(2 * g + 1, 2 * (g + n), 2):
            arrived(tokens.at[slot], mate_recv.at[slot // 2])
        block = tokens[pl.ds(2 * g, 2 * n)].reshape(2 * n * here, width)
        slots = range(2 * g, 2 * (g + n))
        project(
            block, [slot for slot in slots for _ in range(2)], (0, 1) * (2 * n), g * 2 * here,
            tuple((i * half, i % 2, (2 * g + i // 2) * half, half) for i in range(4 * n)),
        )

    def project_late(p, n):
        for q in range(p, p + n):
            arrived(late_tokens.at[q, pl.ds(late_count, late_count)], late_recv.at[1, q])
        size = n * late_size
        block = late_tokens[pl.ds(p, n)].reshape(size, width)
        project(
            block, late_order * n, (p // 2,) * (n * len(late_slots)), EARLY * here + p * late_size,
            ((0, p // 2, EARLY * half + p % 2 * late_size, size),),
        )

    take(left, 0)
    send_piece(left, 0, right, far)
    send_piece(left, 0, partner, partner_left)
    share(left, 0)
    take(partner, 0)
    share(partner, 0)
    take(right, 0)
    send_piece(right, 0, partner, partner_right)
    share(right, 0)
    project_groups(0, 1)
    take(right, 1)
    send_piece(right, 1, left, far)
    share(right, 1)
    take(partner, 1)
    share(partner, 1)
    take(left, 1)
    share(left, 1)
    take(left, 2)
    send_piece(left, 2, right, far)
    share(left, 2)
    take(partner, 2)
    share(partner, 2)
    take(right, 2)
    share(right, 2)
    take(right, 3)
    send_piece(right, 3, left, far)
    share(right, 3)
    for p in (1, 2):
        send_piece(partner, p, left, partner_right)
        send_piece(partner, p, right, partner_left)
    take(partner, 3)
    send_piece(partner, 3, right, partner_left)
    send_piece(partner, 3, left, partner_right)
    share(partner, 3)
    take(left, 3)
    share(left, 3)

    def take_far(p):
        take(far, p)
        if p:
            send_piece(far, p, partner, partner_far)
        share(far, p)

    def pass_on(p, first, n):
        push(
            late_tokens.at[p, pl.ds(first, n)], late_tokens.at[p, pl.ds(late_count + first, n)],
            sent.at[3], late_recv.at[1, p], on_seq(mate),
        )

    def take_pair(p):
        here_already = 0 if p else 1
        arrived(late_tokens.at[p, pl.ds(here_already, 2 - here_already)], late_recv.at[0, p])
        pass_on(p, 0, 2)

    def take_last(p):
        take(partner_far, p)
        pass_on(p, 2, 1)

    take_far(0)
    take(partner_left, 0)
    send_piece(partner_left, 0, right, partner_far)
    take_far(1)
    project_groups(1, 1)
    take_far(2)
    project_groups(2, 2)
    take_far(3)
    take_pair(0)
    take_pair(1)
    project_groups(4, 1)
    take_pair(2)
    take_last(1)
    take_pair(3)
    take_last(0)
    take_last(2)
    take_last(3)
    project_late(0, 2)
    project_late(2, 2)

    factor = scale_ref[0, 0] * math.log2(math.e)

    def scores_of(h, start, size):
        return lax.dot_general(
            query[h, pl.ds(start, size), :], key[...], (((1,), (1,)), ((), ())), preferred_element_type=jnp.float32
        )

    def attend(scores):
        lifted = jnp.exp2((scores - jnp.max(scores, -1, keepdims=True)) * factor)
        mixed = jnp.dot(lifted.astype(jnp.bfloat16), value[...], preferred_element_type=jnp.float32)
        return (mixed / mixed[:, per_head : per_head + 1]).astype(heads.dtype)

    def deliver(slot, h):
        if slot:
            to = back_slot(slot)
            push(heads.at[h, slot], spread.at[h, to], sent.at[4], head_recv.at[h], on_seq(slot))

    middle = count // 2
    blocks = [(h, start) for h in range(2) for start in (middle, 0)]
    upcoming = scores_of(blocks[0][0], blocks[0][1] * half, middle * half)
    for i, (h, start) in enumerate(blocks):
        scores = upcoming
        if i + 1 < len(blocks):
            upcoming = scores_of(blocks[i + 1][0], blocks[i + 1][1] * half, middle * half)
        mixed = attend(scores)
        if start:
            for slot in range(middle, EARLY):
                first = (slot - middle) * half
                heads[h, slot] = mixed[first : first + half]
            for k, slot in enumerate(late_order):
                for p in range(2):
                    first = (EARLY - middle) * half + p * late_size + k * unit
                    heads[h, slot, pl.ds(p * unit, unit), :] = mixed[first : first + unit]
        else:
            heads[h, pl.ds(0, middle)] = mixed.reshape(middle, half, LANES)
            spread[h, 0] = heads[h, 0]
        for slot in reversed(range(start, start + middle)):
            deliver(slot, h)

    span = width // chunks
    pltpu.make_async_copy(out_w_ref, wout, local_sem.at[6]).wait()
    for h in range(2):
        arrived(spread.at[h, pl.ds(1, count - 1)], head_recv.at[h])
        gathered = jnp.concatenate([spread[h, slot][:, :per_head] for slot in range(count)], axis=-1)
        for n in range(chunks):
            attention = jnp.dot(gathered, wout[:, pl.ds(n * span, span)], preferred_element_type=jnp.float32)
            mine[h, n] = attention.astype(mine.dtype)
            for s, device in ((0, after), (1, before)):
                part = pl.ds(s * low, low)
                push(mine.at[h, n, part], theirs.at[h, n, part], sent.at[5], z_recv.at[h, n], device)
    for h in range(2):
        for n in range(chunks):
            rows, columns = pl.ds(h * half, half), pl.ds(n * span, span)
            arrived(theirs.at[h, n], z_recv.at[h, n])
            attention = jnp.where(taken(column), theirs[h, n].astype(jnp.float32), mine[h, n].astype(jnp.float32))
            finished = own[rows, columns].astype(jnp.float32) + gate_row[:, n * span : (n + 1) * span] * attention
            ysend[h, n] = finished.astype(ysend.dtype)
            push(ysend.at[h, n], out_ref.at[rows, columns], sent.at[6], y_recv.at[0], other)
    assert sends[0] == 12 * PIECES
    left_here(own, sent.at[0])
    left_here(tokens, sent.at[1])
    left_here(tokens.at[pl.ds(0, sends[0] // PIECES - EARLY)], sent.at[2])
    left_here(late_tokens.at[:, pl.ds(0, late_count)], sent.at[3])
    left_here(heads.at[:, pl.ds(1, count - 1)], sent.at[4])
    left_here(mine, sent.at[5])
    arrived(out_ref, y_recv.at[0])
    left_here(ysend, sent.at[6])


def shards(
    latents, timesteps, offsets, qkv_weight, logit_scale, out_weight, mod_shift, mod_scale, mod_gate
):
    _, row_count, col_count, width = latents.shape
    wins, seq = lax.axis_size("win"), lax.axis_size("seq")
    here = row_count * col_count
    half = here // 2
    unit = here // PIECES
    steps = mod_shift.shape[1]
    chunks = 3 if width % 384 == 0 else 2
    span = width // chunks
    bf16 = jnp.bfloat16
    in_hbm = pl.BlockSpec(memory_space=pltpu.HBM)
    dma = pltpu.SemaphoreType.DMA
    result = pl.pallas_call(
        functools.partial(fused, wins, chunks),
        out_shape=pltpu.VMEM((here, width), bf16),
        in_specs=[in_hbm] * 9,
        out_specs=pl.BlockSpec(memory_space=pltpu.VMEM),
        scratch_shapes=[
            pltpu.SMEM((1,), jnp.int32),
            pltpu.SMEM((1, 2), jnp.int32),
            pltpu.SMEM((1, 1), jnp.float32),
            pltpu.VMEM((here, width), bf16),
            pltpu.VMEM((here, width), bf16),
            pltpu.VMEM((3, steps, width), jnp.float32),
            pltpu.VMEM((3 * LANES, width), bf16),
            pltpu.VMEM((width, 3 * LANES), bf16),
            pltpu.VMEM((seq * (LANES * 3 // 4), width), bf16),
            pltpu.VMEM((EARLY, here, width), bf16),
            pltpu.VMEM((PIECES, seq - EARLY, unit, width), bf16),
            pltpu.VMEM((2, seq * half, LANES), bf16),
            pltpu.VMEM((seq * here, LANES), bf16),
            pltpu.VMEM((seq * here, LANES), bf16),
            pltpu.VMEM((2, seq, half, LANES), bf16),
            pltpu.VMEM((2, seq, half, LANES), bf16),
            pltpu.VMEM((2, chunks, half, span), bf16),
            pltpu.VMEM((2, chunks, half, span), bf16),
            pltpu.VMEM((2, chunks, half, span), bf16),
            dma((7,)),
            dma((7,)),
            dma((2,)),
            dma((EARLY // 2, PIECES)),
            dma((EARLY // 2,)),
            dma((2, PIECES)),
            dma((PIECES + 1,)),
            dma((2,)),
            dma((2, chunks)),
            dma((1,)),
        ],
        compiler_params=pltpu.CompilerParams(
            collective_id=0, has_side_effects=True, vmem_limit_bytes=56 * 1024 * 1024
        ),
    )(
        latents.reshape(here, width),
        timesteps,
        offsets,
        qkv_weight[0, :, 0, :].T,
        logit_scale,
        out_weight[0],
        mod_shift[0],
        mod_scale[0],
        mod_gate[0],
    )
    return result.reshape(1, row_count, col_count, width)


def solution(mesh):
    in_specs = (
        P("segment", "seq", "win", None),
        P("segment"),
        P("segment", None),
        P("segment", None, "seq", None),
        P("segment", "seq"),
        P("segment", None, None),
        P("segment", None, None),
        P("segment", None, None),
        P("segment", None, None),
    )
    out_specs = P("segment", "seq", "win", None)
    return jax.shard_map(shards, mesh=mesh, in_specs=in_specs, out_specs=out_specs, check_vma=False)
```

```python
import functools
import math

import jax
import jax.numpy as jnp
from jax import lax
from jax.experimental import pallas as pl
from jax.experimental.pallas import tpu as pltpu
from jax.sharding import PartitionSpec as P

eps_norm = 1e-06
far_apart = 32768.0
LANES = 128
X_CHIPS = 4
Y_CHIPS = 2
PIECES = 4
EARLY = 10
MESH = pl.DeviceIdType.MESH

GROUPS = ((0, 0), (3, 0), (1, 0), (0, 1), (2, 0), (3, 1), (1, 1), (2, 1))


def slot_of(dx, dy, dc):
    return 2 * GROUPS.index((dx % X_CHIPS, dy % Y_CHIPS)) + dc % 2


def back_slot(slot):
    dx, dy = GROUPS[slot // 2]
    return slot_of(-dx, -dy, slot % 2)


def fused(
    wins, chunks,
    tile_ref, level_hbm, offset_hbm, qkv_ref, scale_hbm, out_w_ref, shift_tab, scale_tab, gate_tab,
    out_ref,
    level_ref, offset_ref, scale_ref,
    own, beside, tabs, wqkv, wmix, wout, tokens, late_tokens, query, key, value, heads, spread, mine, theirs, ysend,
    local_sem, sent, in_recv, recv_sem, mate_recv, late_recv, far_recv, head_recv, z_recv, y_recv,
):
    me = lax.axis_index("seq")
    win = lax.axis_index("win")
    segment = lax.axis_index("segment")
    core = lax.rem(me, 2)
    x = lax.rem(me // 2, X_CHIPS)
    y = me // (2 * X_CHIPS)

    def seq_of(slot):
        dx, dy = GROUPS[slot // 2]
        chip = lax.rem(y + dy, Y_CHIPS) * X_CHIPS + lax.rem(x + dx, X_CHIPS)
        return 2 * chip + lax.rem(core + slot % 2, 2)

    def on_seq(slot):
        return {"seq": seq_of(slot)}

    right, left, partner, mate = slot_of(1, 0, 0), slot_of(3, 0, 0), slot_of(0, 1, 0), slot_of(0, 0, 1)
    far, partner_left, partner_right, partner_far = slot_of(2, 0, 0), slot_of(3, 1, 0), slot_of(1, 1, 0), slot_of(2, 1, 0)
    after = {"win": lax.rem(win + 1, wins)}
    before = {"win": lax.rem(win + wins - 1, wins)}
    other = {"segment": 1 - segment}
    across = {"segment": 1 - segment, "seq": seq_of(partner)}

    width = own.shape[1]
    here = own.shape[0]
    half = here // 2
    low = half // 2
    unit = here // PIECES
    per_head = LANES * 3 // 4
    count = spread.shape[1]

    pltpu.make_async_copy(tile_ref, own, local_sem.at[0]).start()
    for i, tab in enumerate((shift_tab, scale_tab, gate_tab)):
        pltpu.make_async_copy(tab, tabs.at[i], local_sem.at[1]).start()
    for i in range(3):
        pltpu.make_async_copy(
            qkv_ref.at[pl.ds(i * per_head, per_head)], wqkv.at[pl.ds(i * LANES, per_head)], local_sem.at[2]
        ).start()
    scalars = [
        pltpu.make_async_copy(src, dst, local_sem.at[3 + i])
        for i, (src, dst) in enumerate(((level_hbm, level_ref), (offset_hbm, offset_ref), (scale_hbm, scale_ref)))
    ]
    for copy in scalars:
        copy.start()

    barrier = pltpu.get_barrier_semaphore()
    greeted = [after, before, across] + [on_seq(s) for s in (right, left, partner, mate)]
    for device in greeted:
        pl.semaphore_signal(barrier, inc=1, device_id=device, device_id_type=MESH)

    for slot in range(count):
        first = pl.multiple_of(seq_of(slot) * per_head, per_head)
        pltpu.make_async_copy(
            out_w_ref.at[pl.ds(first, per_head)], wout.at[pl.ds(slot * per_head, per_head)], local_sem.at[6]
        ).start()
    pltpu.make_async_copy(tile_ref, own, local_sem.at[0]).wait()
    pl.semaphore_wait(barrier, len(greeted))

    def push(src, dst, send, recv, device):
        pltpu.make_async_remote_copy(
            src_ref=src, dst_ref=dst, send_sem=send, recv_sem=recv, device_id=device, device_id_type=MESH
        ).start()

    def arrived(ref, sem):
        pltpu.make_async_remote_copy(
            src_ref=ref, dst_ref=ref, send_sem=sent.at[0], recv_sem=sem, device_id=after, device_id_type=MESH
        ).wait_recv()

    def left_here(ref, sem):
        pltpu.make_async_remote_copy(
            src_ref=ref, dst_ref=ref, send_sem=sem, recv_sem=in_recv.at[0], device_id=after, device_id_type=MESH
        ).wait_send()

    sides = ((0, before), (1, after))
    for h in range(2):
        for s, device in sides:
            part = pl.ds(h * half + s * low, low)
            push(own.at[part], beside.at[part], sent.at[0], in_recv.at[h], device)

    for i in range(3):
        wqkv[pl.ds(i * LANES + per_head, LANES - per_head), :] = jnp.zeros((LANES - per_head, width), wqkv.dtype)
    pltpu.make_async_copy(qkv_ref, wqkv.at[pl.ds(0, 3 * per_head)], local_sem.at[2]).wait()
    wmix[...] = wqkv[...].T
    for copy in scalars:
        copy.wait()
    level = level_ref[0]
    lat_offset = offset_ref[0, 0]
    lon_offset = offset_ref[0, 1]
    pltpu.make_async_copy(tabs, tabs, local_sem.at[1]).wait()
    shift_row = tabs[0, pl.ds(level, 1), :]
    scale_row = tabs[1, pl.ds(level, 1), :]
    gate_row = tabs[2, pl.ds(level, 1), :]
    column = lax.broadcasted_iota(jnp.int32, (half, 1), 0)
    low_end = jnp.where(lon_offset <= low, lon_offset, 0)
    high_start = jnp.where(lon_offset <= low, half, lon_offset)

    def taken(column):
        return jnp.logical_or(column < low_end, column >= high_start)

    late_slots = tuple(range(EARLY, count))
    late_count = len(late_slots) // 2
    sends = [0]

    def piece(slot, p):
        if slot < EARLY:
            return tokens.at[slot, pl.ds(p * unit, unit)]
        return late_tokens.at[slot % 2, p, late_slots.index(slot) // 2]

    def arrival(slot, p):
        if (slot, p) == (partner_left, 0):
            return far_recv.at[PIECES]
        if slot == partner_far:
            return far_recv.at[p]
        if slot >= EARLY:
            return late_recv.at[p]
        return mate_recv.at[slot // 2] if slot % 2 else recv_sem.at[slot // 2 - 1, p]

    def send_piece(src_slot, p, device_slot, dst_slot):
        lot = 1 if sends[0] < EARLY * PIECES else 2
        push(piece(src_slot, p), piece(dst_slot, p), sent.at[lot], arrival(dst_slot, p), on_seq(device_slot))
        sends[0] += 1

    for h in range(2):
        part = pl.ds(h * half, half)
        arrived(beside.at[part], in_recv.at[h])
        rows = jnp.where(taken(column), beside[part, :].astype(jnp.float32), own[part, :].astype(jnp.float32))
        centred = rows - jnp.mean(rows, -1, keepdims=True)
        variance = jnp.mean(centred * centred, -1, keepdims=True)
        normed = centred * lax.rsqrt(variance + eps_norm) * scale_row + shift_row
        tokens[0, part, :] = normed.astype(tokens.dtype)
        for p in (2 * h, 2 * h + 1):
            send_piece(0, p, partner, partner)
            send_piece(0, p, right, left)
            send_piece(0, p, left, right)
        for p in (2 * h, 2 * h + 1):
            send_piece(0, p, mate, mate)

    def take(slot, p):
        arrived(piece(slot, p), arrival(slot, p))

    def share(slot, p):
        send_piece(slot, p, mate, slot + 1)

    def project(block, owners, parities, start, places):
        size = block.shape[0]
        each = size // len(owners)
        mixed = jnp.dot(block, wmix[...], preferred_element_type=jnp.float32)
        q = mixed[:, :LANES]
        k = mixed[:, LANES : 2 * LANES]
        v = mixed[:, 2 * LANES :]
        q = q * lax.rsqrt(jnp.sum(q * q, -1, keepdims=True) + eps_norm)
        k = k * lax.rsqrt(jnp.sum(k * k, -1, keepdims=True) + eps_norm)
        lane = lax.broadcasted_iota(jnp.int32, (size, LANES), 1)
        index = lax.broadcasted_iota(jnp.int32, (size, LANES), 0)
        row = jnp.zeros((size, LANES), jnp.int32)
        for i, (slot, parity) in enumerate(zip(owners, parities)):
            row = jnp.where(index >= i * each, 2 * seq_of(slot) + parity, row)
        late = row >= lat_offset
        q = jnp.where(lane == per_head, jnp.where(late, 1.0, 0.0), q)
        q = jnp.where(lane == per_head + 1, jnp.where(late, 0.0, 1.0), q)
        k = jnp.where(lane == per_head, jnp.where(late, 0.0, -far_apart), k)
        k = jnp.where(lane == per_head + 1, jnp.where(late, -far_apart, 0.0), k)
        v = jnp.where(lane == per_head, 1.0, v)
        q = q.astype(query.dtype)
        for first, h, place, extent in places:
            query[h, pl.ds(place, extent), :] = q[first : first + extent]
        at = pl.ds(start, size)
        key[at, :] = k.astype(key.dtype)
        value[at, :] = v.astype(value.dtype)

    def project_groups(g, n):
        for slot in range(2 * g + 1, 2 * (g + n), 2):
            arrived(tokens.at[slot], mate_recv.at[slot // 2])
        block = tokens[pl.ds(2 * g, 2 * n)].reshape(2 * n * here, width)
        slots = range(2 * g, 2 * (g + n))
        project(
            block, [slot for slot in slots for _ in range(2)], (0, 1) * (2 * n), g * 2 * here,
            tuple((i * half, i % 2, (2 * g + i // 2) * half, half) for i in range(4 * n)),
        )

    def project_late(lane):
        size = PIECES * late_count * unit
        pair = size // 2
        project(
            late_tokens[lane].reshape(size, width), late_slots[lane::2] * PIECES,
            [p // 2 for p in range(PIECES) for _ in range(late_count)], EARLY * here + lane * size,
            tuple((h * pair, h, EARLY * half + lane * pair, pair) for h in range(2)),
        )

    take(left, 0)
    send_piece(left, 0, right, far)
    send_piece(left, 0, partner, partner_left)
    share(left, 0)
    take(partner, 0)
    share(partner, 0)
    take(right, 0)
    send_piece(right, 0, partner, partner_right)
    share(right, 0)
    project_groups(0, 1)
    take(right, 1)
    send_piece(right, 1, left, far)
    share(right, 1)
    take(partner, 1)
    share(partner, 1)
    take(left, 1)
    share(left, 1)
    take(left, 2)
    send_piece(left, 2, right, far)
    share(left, 2)
    take(partner, 2)
    share(partner, 2)
    take(right, 2)
    share(right, 2)
    take(right, 3)
    send_piece(right, 3, left, far)
    share(right, 3)
    for p in (1, 2):
        send_piece(partner, p, left, partner_right)
        send_piece(partner, p, right, partner_left)
    take(partner, 3)
    send_piece(partner, 3, right, partner_left)
    send_piece(partner, 3, left, partner_right)
    share(partner, 3)
    take(left, 3)
    share(left, 3)

    def take_far(p):
        take(far, p)
        if p:
            send_piece(far, p, partner, partner_far)
        share(far, p)

    def pass_on(p, first, n):
        push(
            late_tokens.at[0, p, pl.ds(first, n)], late_tokens.at[1, p, pl.ds(first, n)],
            sent.at[3], late_recv.at[PIECES], on_seq(mate),
        )

    def take_pair(p):
        here_already = 0 if p else 1
        arrived(late_tokens.at[0, p, pl.ds(here_already, 2 - here_already)], late_recv.at[p])
        pass_on(p, 0, 2)

    def take_last(p):
        take(partner_far, p)
        pass_on(p, 2, 1)

    take_far(0)
    take(partner_left, 0)
    send_piece(partner_left, 0, right, partner_far)
    take_far(1)
    project_groups(1, 1)
    take_far(2)
    project_groups(2, 2)
    take_far(3)
    take_pair(0)
    take_pair(1)
    project_groups(4, 1)
    take_pair(2)
    take_last(1)
    take_pair(3)
    take_last(0)
    take_last(2)
    take_last(3)
    project_late(0)
    arrived(late_tokens.at[1], late_recv.at[PIECES])
    project_late(1)

    factor = scale_ref[0, 0] * math.log2(math.e)

    def scores_of(h, start, size):
        return lax.dot_general(
            query[h, pl.ds(start, size), :], key[...], (((1,), (1,)), ((), ())), preferred_element_type=jnp.float32
        )

    def attend(scores):
        lifted = jnp.exp2((scores - jnp.max(scores, -1, keepdims=True)) * factor)
        mixed = jnp.dot(lifted.astype(jnp.bfloat16), value[...], preferred_element_type=jnp.float32)
        return (mixed / mixed[:, per_head : per_head + 1]).astype(heads.dtype)

    def deliver(slot, h):
        if slot:
            to = back_slot(slot)
            push(heads.at[h, slot], spread.at[h, to], sent.at[4], head_recv.at[h], on_seq(slot))

    middle = count // 2
    blocks = [(h, start) for h in range(2) for start in (middle, 0)]
    upcoming = scores_of(blocks[0][0], blocks[0][1] * half, middle * half)
    for i, (h, start) in enumerate(blocks):
        scores = upcoming
        if i + 1 < len(blocks):
            upcoming = scores_of(blocks[i + 1][0], blocks[i + 1][1] * half, middle * half)
        mixed = attend(scores)
        if start:
            for slot in range(middle, EARLY):
                first = (slot - middle) * half
                heads[h, slot] = mixed[first : first + half]
            for slot in late_slots:
                for p in range(2):
                    first = (EARLY - middle) * half + ((slot % 2 * 2 + p) * late_count + (slot - EARLY) // 2) * unit
                    heads[h, slot, pl.ds(p * unit, unit), :] = mixed[first : first + unit]
        else:
            heads[h, pl.ds(0, middle)] = mixed.reshape(middle, half, LANES)
            spread[h, 0] = heads[h, 0]
        for slot in reversed(range(start, start + middle)):
            deliver(slot, h)

    span = width // chunks
    pltpu.make_async_copy(out_w_ref, wout, local_sem.at[6]).wait()
    for h in range(2):
        arrived(spread.at[h, pl.ds(1, count - 1)], head_recv.at[h])
        gathered = jnp.concatenate([spread[h, slot][:, :per_head] for slot in range(count)], axis=-1)
        for n in range(chunks):
            attention = jnp.dot(gathered, wout[:, pl.ds(n * span, span)], preferred_element_type=jnp.float32)
            mine[h, n] = attention.astype(mine.dtype)
            for s, device in ((0, after), (1, before)):
                part = pl.ds(s * low, low)
                push(mine.at[h, n, part], theirs.at[h, n, part], sent.at[5], z_recv.at[h, n], device)
    for h in range(2):
        for n in range(chunks):
            rows, columns = pl.ds(h * half, half), pl.ds(n * span, span)
            arrived(theirs.at[h, n], z_recv.at[h, n])
            attention = jnp.where(taken(column), theirs[h, n].astype(jnp.float32), mine[h, n].astype(jnp.float32))
            finished = own[rows, columns].astype(jnp.float32) + gate_row[:, n * span : (n + 1) * span] * attention
            ysend[h, n] = finished.astype(ysend.dtype)
            push(ysend.at[h, n], out_ref.at[rows, columns], sent.at[6], y_recv.at[0], other)
    assert sends[0] == 12 * PIECES
    left_here(own, sent.at[0])
    left_here(tokens, sent.at[1])
    left_here(tokens.at[pl.ds(0, sends[0] // PIECES - EARLY)], sent.at[2])
    left_here(late_tokens.at[0], sent.at[3])
    left_here(heads.at[:, pl.ds(1, count - 1)], sent.at[4])
    left_here(mine, sent.at[5])
    arrived(out_ref, y_recv.at[0])
    left_here(ysend, sent.at[6])


def shards(
    latents, timesteps, offsets, qkv_weight, logit_scale, out_weight, mod_shift, mod_scale, mod_gate
):
    _, row_count, col_count, width = latents.shape
    wins, seq = lax.axis_size("win"), lax.axis_size("seq")
    here = row_count * col_count
    half = here // 2
    unit = here // PIECES
    steps = mod_shift.shape[1]
    chunks = 3 if width % 384 == 0 else 2
    span = width // chunks
    bf16 = jnp.bfloat16
    in_hbm = pl.BlockSpec(memory_space=pltpu.HBM)
    dma = pltpu.SemaphoreType.DMA
    result = pl.pallas_call(
        functools.partial(fused, wins, chunks),
        out_shape=pltpu.VMEM((here, width), bf16),
        in_specs=[in_hbm] * 9,
        out_specs=pl.BlockSpec(memory_space=pltpu.VMEM),
        scratch_shapes=[
            pltpu.SMEM((1,), jnp.int32),
            pltpu.SMEM((1, 2), jnp.int32),
            pltpu.SMEM((1, 1), jnp.float32),
            pltpu.VMEM((here, width), bf16),
            pltpu.VMEM((here, width), bf16),
            pltpu.VMEM((3, steps, width), jnp.float32),
            pltpu.VMEM((3 * LANES, width), bf16),
            pltpu.VMEM((width, 3 * LANES), bf16),
            pltpu.VMEM((seq * (LANES * 3 // 4), width), bf16),
            pltpu.VMEM((EARLY, here, width), bf16),
            pltpu.VMEM((2, PIECES, (seq - EARLY) // 2, unit, width), bf16),
            pltpu.VMEM((2, seq * half, LANES), bf16),
            pltpu.VMEM((seq * here, LANES), bf16),
            pltpu.VMEM((seq * here, LANES), bf16),
            pltpu.VMEM((2, seq, half, LANES), bf16),
            pltpu.VMEM((2, seq, half, LANES), bf16),
            pltpu.VMEM((2, chunks, half, span), bf16),
            pltpu.VMEM((2, chunks, half, span), bf16),
            pltpu.VMEM((2, chunks, half, span), bf16),
            dma((7,)),
            dma((7,)),
            dma((2,)),
            dma((EARLY // 2 - 1, PIECES)),
            dma((EARLY // 2,)),
            dma((PIECES + 1,)),
            dma((PIECES + 1,)),
            dma((2,)),
            dma((2, chunks)),
            dma((1,)),
        ],
        compiler_params=pltpu.CompilerParams(
            collective_id=0, has_side_effects=True, vmem_limit_bytes=56 * 1024 * 1024
        ),
    )(
        latents.reshape(here, width),
        timesteps,
        offsets,
        qkv_weight[0, :, 0, :].T,
        logit_scale,
        out_weight[0],
        mod_shift[0],
        mod_scale[0],
        mod_gate[0],
    )
    return result.reshape(1, row_count, col_count, width)


def solution(mesh):
    in_specs = (
        P("segment", "seq", "win", None),
        P("segment"),
        P("segment", None),
        P("segment", None, "seq", None),
        P("segment", "seq"),
        P("segment", None, None),
        P("segment", None, None),
        P("segment", None, None),
        P("segment", None, None),
    )
    out_specs = P("segment", "seq", "win", None)
    return jax.shard_map(shards, mesh=mesh, in_specs=in_specs, out_specs=out_specs, check_vma=False)
```

```python
import functools
import math

import jax
import jax.numpy as jnp
from jax import lax
from jax.experimental import pallas as pl
from jax.experimental.pallas import tpu as pltpu
from jax.sharding import PartitionSpec as P

eps_norm = 1e-06
far_apart = 32768.0
LANES = 128
X_CHIPS = 4
Y_CHIPS = 2
PIECES = 4
EARLY = 10
MESH = pl.DeviceIdType.MESH

GROUPS = ((0, 0), (3, 0), (1, 0), (0, 1), (2, 0), (3, 1), (1, 1), (2, 1))


def slot_of(dx, dy, dc):
    return 2 * GROUPS.index((dx % X_CHIPS, dy % Y_CHIPS)) + dc % 2


def back_slot(slot):
    dx, dy = GROUPS[slot // 2]
    return slot_of(-dx, -dy, slot % 2)


def fused(
    wins, chunks,
    tile_ref, level_hbm, offset_hbm, qkv_ref, scale_hbm, out_w_ref, shift_tab, scale_tab, gate_tab,
    out_ref,
    level_ref, offset_ref, scale_ref,
    own, beside, tabs, wqkv, wmix, wout, tokens, late_tokens, query, key, value, heads, spread, mine, theirs, ysend,
    local_sem, sent, in_recv, recv_sem, mate_recv, late_recv, far_recv, head_recv, z_recv, y_recv,
):
    me = lax.axis_index("seq")
    win = lax.axis_index("win")
    segment = lax.axis_index("segment")
    core = lax.rem(me, 2)
    x = lax.rem(me // 2, X_CHIPS)
    y = me // (2 * X_CHIPS)

    def seq_of(slot):
        dx, dy = GROUPS[slot // 2]
        chip = lax.rem(y + dy, Y_CHIPS) * X_CHIPS + lax.rem(x + dx, X_CHIPS)
        return 2 * chip + lax.rem(core + slot % 2, 2)

    def on_seq(slot):
        return {"seq": seq_of(slot)}

    right, left, partner, mate = slot_of(1, 0, 0), slot_of(3, 0, 0), slot_of(0, 1, 0), slot_of(0, 0, 1)
    far, partner_left, partner_right, partner_far = slot_of(2, 0, 0), slot_of(3, 1, 0), slot_of(1, 1, 0), slot_of(2, 1, 0)
    after = {"win": lax.rem(win + 1, wins)}
    before = {"win": lax.rem(win + wins - 1, wins)}
    other = {"segment": 1 - segment}
    across = {"segment": 1 - segment, "seq": seq_of(partner)}

    width = own.shape[1]
    here = own.shape[0]
    half = here // 2
    low = half // 2
    unit = here // PIECES
    per_head = LANES * 3 // 4
    count = spread.shape[1]

    pltpu.make_async_copy(tile_ref, own, local_sem.at[0]).start()
    for i, tab in enumerate((shift_tab, scale_tab, gate_tab)):
        pltpu.make_async_copy(tab, tabs.at[i], local_sem.at[1]).start()
    for i in range(3):
        pltpu.make_async_copy(
            qkv_ref.at[pl.ds(i * per_head, per_head)], wqkv.at[pl.ds(i * LANES, per_head)], local_sem.at[2]
        ).start()
    scalars = [
        pltpu.make_async_copy(src, dst, local_sem.at[3 + i])
        for i, (src, dst) in enumerate(((level_hbm, level_ref), (offset_hbm, offset_ref), (scale_hbm, scale_ref)))
    ]
    for copy in scalars:
        copy.start()

    barrier = pltpu.get_barrier_semaphore()
    greeted = [after, before, across] + [on_seq(s) for s in (right, left, partner, mate)]
    for device in greeted:
        pl.semaphore_signal(barrier, inc=1, device_id=device, device_id_type=MESH)

    for slot in range(count):
        first = pl.multiple_of(seq_of(slot) * per_head, per_head)
        pltpu.make_async_copy(
            out_w_ref.at[pl.ds(first, per_head)], wout.at[pl.ds(slot * per_head, per_head)], local_sem.at[6]
        ).start()
    pltpu.make_async_copy(tile_ref, own, local_sem.at[0]).wait()
    pl.semaphore_wait(barrier, len(greeted))

    def push(src, dst, send, recv, device):
        pltpu.make_async_remote_copy(
            src_ref=src, dst_ref=dst, send_sem=send, recv_sem=recv, device_id=device, device_id_type=MESH
        ).start()

    def arrived(ref, sem):
        pltpu.make_async_remote_copy(
            src_ref=ref, dst_ref=ref, send_sem=sent.at[0], recv_sem=sem, device_id=after, device_id_type=MESH
        ).wait_recv()

    def left_here(ref, sem):
        pltpu.make_async_remote_copy(
            src_ref=ref, dst_ref=ref, send_sem=sem, recv_sem=in_recv.at[0], device_id=after, device_id_type=MESH
        ).wait_send()

    sides = ((0, before), (1, after))
    for h in range(2):
        for s, device in sides:
            part = pl.ds(h * half + s * low, low)
            push(own.at[part], beside.at[part], sent.at[0], in_recv.at[h], device)

    for i in range(3):
        wqkv[pl.ds(i * LANES + per_head, LANES - per_head), :] = jnp.zeros((LANES - per_head, width), wqkv.dtype)
    pltpu.make_async_copy(qkv_ref, wqkv.at[pl.ds(0, 3 * per_head)], local_sem.at[2]).wait()
    wmix[...] = wqkv[...].T
    for copy in scalars:
        copy.wait()
    level = level_ref[0]
    lat_offset = offset_ref[0, 0]
    lon_offset = offset_ref[0, 1]
    pltpu.make_async_copy(tabs, tabs, local_sem.at[1]).wait()
    shift_row = tabs[0, pl.ds(level, 1), :]
    scale_row = tabs[1, pl.ds(level, 1), :]
    gate_row = tabs[2, pl.ds(level, 1), :]
    column = lax.broadcasted_iota(jnp.int32, (half, 1), 0)
    low_end = jnp.where(lon_offset <= low, lon_offset, 0)
    high_start = jnp.where(lon_offset <= low, half, lon_offset)

    def taken(column):
        return jnp.logical_or(column < low_end, column >= high_start)

    late_slots = tuple(range(EARLY, count))
    late_count = len(late_slots) // 2
    sends = [0]

    def piece(slot, p):
        if slot < EARLY:
            return tokens.at[slot, pl.ds(p * unit, unit)]
        return late_tokens.at[slot % 2, p, late_slots.index(slot) // 2]

    def arrival(slot, p):
        if (slot, p) == (partner_left, 0):
            return far_recv.at[PIECES]
        if slot == partner_far:
            return far_recv.at[p]
        if slot >= EARLY:
            return late_recv.at[p]
        return mate_recv.at[slot // 2] if slot % 2 else recv_sem.at[slot // 2 - 1, p]

    def send_piece(src_slot, p, device_slot, dst_slot):
        lot = 1 if sends[0] < EARLY * PIECES else 2
        push(piece(src_slot, p), piece(dst_slot, p), sent.at[lot], arrival(dst_slot, p), on_seq(device_slot))
        sends[0] += 1

    for h in range(2):
        part = pl.ds(h * half, half)
        arrived(beside.at[part], in_recv.at[h])
        rows = jnp.where(taken(column), beside[part, :].astype(jnp.float32), own[part, :].astype(jnp.float32))
        centred = rows - jnp.mean(rows, -1, keepdims=True)
        variance = jnp.mean(centred * centred, -1, keepdims=True)
        normed = centred * lax.rsqrt(variance + eps_norm) * scale_row + shift_row
        tokens[0, part, :] = normed.astype(tokens.dtype)
        for p in (2 * h, 2 * h + 1):
            send_piece(0, p, partner, partner)
            send_piece(0, p, right, left)
            send_piece(0, p, left, right)
        for p in (2 * h, 2 * h + 1):
            send_piece(0, p, mate, mate)

    def take(slot, p):
        arrived(piece(slot, p), arrival(slot, p))

    def share(slot, p):
        send_piece(slot, p, mate, slot + 1)

    def project(block, owners, parities, start, places):
        size = block.shape[0]
        each = size // len(owners)
        mixed = jnp.dot(block, wmix[...], preferred_element_type=jnp.float32)
        q = mixed[:, :LANES]
        k = mixed[:, LANES : 2 * LANES]
        v = mixed[:, 2 * LANES :]
        q = q * lax.rsqrt(jnp.sum(q * q, -1, keepdims=True) + eps_norm)
        k = k * lax.rsqrt(jnp.sum(k * k, -1, keepdims=True) + eps_norm)
        lane = lax.broadcasted_iota(jnp.int32, (size, LANES), 1)
        index = lax.broadcasted_iota(jnp.int32, (size, LANES), 0)
        row = jnp.zeros((size, LANES), jnp.int32)
        for i, (slot, parity) in enumerate(zip(owners, parities)):
            row = jnp.where(index >= i * each, 2 * seq_of(slot) + parity, row)
        late = row >= lat_offset
        q = jnp.where(lane == per_head, jnp.where(late, 1.0, 0.0), q)
        q = jnp.where(lane == per_head + 1, jnp.where(late, 0.0, 1.0), q)
        k = jnp.where(lane == per_head, jnp.where(late, 0.0, -far_apart), k)
        k = jnp.where(lane == per_head + 1, jnp.where(late, -far_apart, 0.0), k)
        v = jnp.where(lane == per_head, 1.0, v)
        q = q.astype(query.dtype)
        for first, h, place, extent in places:
            query[h, pl.ds(place, extent), :] = q[first : first + extent]
        at = pl.ds(start, size)
        key[at, :] = k.astype(key.dtype)
        value[at, :] = v.astype(value.dtype)

    def project_groups(g, n):
        for slot in range(2 * g + 1, 2 * (g + n), 2):
            arrived(tokens.at[slot], mate_recv.at[slot // 2])
        block = tokens[pl.ds(2 * g, 2 * n)].reshape(2 * n * here, width)
        slots = range(2 * g, 2 * (g + n))
        project(
            block, [slot for slot in slots for _ in range(2)], (0, 1) * (2 * n), g * 2 * here,
            tuple((i * half, i % 2, (2 * g + i // 2) * half, half) for i in range(4 * n)),
        )

    def project_late(lane):
        size = PIECES * late_count * unit
        pair = size // 2
        project(
            late_tokens[lane].reshape(size, width), late_slots[lane::2] * PIECES,
            [p // 2 for p in range(PIECES) for _ in range(late_count)], EARLY * here + lane * size,
            tuple((h * pair, h, EARLY * half + lane * pair, pair) for h in range(2)),
        )

    take(left, 0)
    send_piece(left, 0, right, far)
    send_piece(left, 0, partner, partner_left)
    share(left, 0)
    take(partner, 0)
    share(partner, 0)
    take(right, 0)
    send_piece(right, 0, partner, partner_right)
    share(right, 0)
    project_groups(0, 1)
    take(right, 1)
    send_piece(right, 1, left, far)
    share(right, 1)
    take(partner, 1)
    share(partner, 1)
    take(left, 1)
    share(left, 1)
    take(left, 2)
    send_piece(left, 2, right, far)
    share(left, 2)
    take(partner, 2)
    share(partner, 2)
    take(right, 2)
    share(right, 2)
    take(right, 3)
    send_piece(right, 3, left, far)
    share(right, 3)
    for p in (1, 2):
        send_piece(partner, p, left, partner_right)
        send_piece(partner, p, right, partner_left)
    take(partner, 3)
    send_piece(partner, 3, right, partner_left)
    send_piece(partner, 3, left, partner_right)
    share(partner, 3)
    take(left, 3)
    share(left, 3)

    def take_far(p):
        take(far, p)
        if p:
            send_piece(far, p, partner, partner_far)
        share(far, p)

    def pass_on(p, first, n):
        push(
            late_tokens.at[0, p, pl.ds(first, n)], late_tokens.at[1, p, pl.ds(first, n)],
            sent.at[3], late_recv.at[PIECES], on_seq(mate),
        )

    def take_pair(p):
        here_already = 0 if p else 1
        arrived(late_tokens.at[0, p, pl.ds(here_already, 2 - here_already)], late_recv.at[p])
        pass_on(p, 0, 2)

    def take_last(p):
        take(partner_far, p)
        pass_on(p, 2, 1)

    take_far(0)
    take(partner_left, 0)
    send_piece(partner_left, 0, right, partner_far)
    take_far(1)
    take_far(2)
    project_groups(1, 1)
    take_far(3)
    project_groups(2, 2)
    take_pair(0)
    take_pair(1)
    project_groups(4, 1)
    take_pair(2)
    take_last(1)
    take_pair(3)
    take_last(0)
    take_last(2)
    take_last(3)
    project_late(0)
    arrived(late_tokens.at[1], late_recv.at[PIECES])
    project_late(1)

    factor = scale_ref[0, 0] * math.log2(math.e)

    def scores_of(h, start, size):
        return lax.dot_general(
            query[h, pl.ds(start, size), :], key[...], (((1,), (1,)), ((), ())), preferred_element_type=jnp.float32
        )

    def attend(scores):
        lifted = jnp.exp2((scores - jnp.max(scores, -1, keepdims=True)) * factor)
        mixed = jnp.dot(lifted.astype(jnp.bfloat16), value[...], preferred_element_type=jnp.float32)
        return (mixed / mixed[:, per_head : per_head + 1]).astype(heads.dtype)

    def deliver(slot, h):
        if slot:
            to = back_slot(slot)
            push(heads.at[h, slot], spread.at[h, to], sent.at[4], head_recv.at[h], on_seq(slot))

    middle = count // 2
    blocks = [(h, start) for h in range(2) for start in (middle, 0)]
    upcoming = scores_of(blocks[0][0], blocks[0][1] * half, middle * half)
    for i, (h, start) in enumerate(blocks):
        scores = upcoming
        if i + 1 < len(blocks):
            upcoming = scores_of(blocks[i + 1][0], blocks[i + 1][1] * half, middle * half)
        mixed = attend(scores)
        if start:
            for slot in range(middle, EARLY):
                first = (slot - middle) * half
                heads[h, slot] = mixed[first : first + half]
            for slot in late_slots:
                for p in range(2):
                    first = (EARLY - middle) * half + ((slot % 2 * 2 + p) * late_count + (slot - EARLY) // 2) * unit
                    heads[h, slot, pl.ds(p * unit, unit), :] = mixed[first : first + unit]
        else:
            heads[h, pl.ds(0, middle)] = mixed.reshape(middle, half, LANES)
            spread[h, 0] = heads[h, 0]
        for slot in reversed(range(start, start + middle)):
            deliver(slot, h)

    span = width // chunks
    pltpu.make_async_copy(out_w_ref, wout, local_sem.at[6]).wait()
    for h in range(2):
        arrived(spread.at[h, pl.ds(1, count - 1)], head_recv.at[h])
        gathered = jnp.concatenate([spread[h, slot][:, :per_head] for slot in range(count)], axis=-1)
        for n in range(chunks):
            attention = jnp.dot(gathered, wout[:, pl.ds(n * span, span)], preferred_element_type=jnp.float32)
            mine[h, n] = attention.astype(mine.dtype)
            for s, device in ((0, after), (1, before)):
                part = pl.ds(s * low, low)
                push(mine.at[h, n, part], theirs.at[h, n, part], sent.at[5], z_recv.at[h, n], device)
    for h in range(2):
        for n in range(chunks):
            rows, columns = pl.ds(h * half, half), pl.ds(n * span, span)
            arrived(theirs.at[h, n], z_recv.at[h, n])
            attention = jnp.where(taken(column), theirs[h, n].astype(jnp.float32), mine[h, n].astype(jnp.float32))
            finished = own[rows, columns].astype(jnp.float32) + gate_row[:, n * span : (n + 1) * span] * attention
            ysend[h, n] = finished.astype(ysend.dtype)
            push(ysend.at[h, n], out_ref.at[rows, columns], sent.at[6], y_recv.at[0], other)
    assert sends[0] == 12 * PIECES
    left_here(own, sent.at[0])
    left_here(tokens, sent.at[1])
    left_here(tokens.at[pl.ds(0, sends[0] // PIECES - EARLY)], sent.at[2])
    left_here(late_tokens.at[0], sent.at[3])
    left_here(heads.at[:, pl.ds(1, count - 1)], sent.at[4])
    left_here(mine, sent.at[5])
    arrived(out_ref, y_recv.at[0])
    left_here(ysend, sent.at[6])


def shards(
    latents, timesteps, offsets, qkv_weight, logit_scale, out_weight, mod_shift, mod_scale, mod_gate
):
    _, row_count, col_count, width = latents.shape
    wins, seq = lax.axis_size("win"), lax.axis_size("seq")
    here = row_count * col_count
    half = here // 2
    unit = here // PIECES
    steps = mod_shift.shape[1]
    chunks = 3 if width % 384 == 0 else 2
    span = width // chunks
    bf16 = jnp.bfloat16
    in_hbm = pl.BlockSpec(memory_space=pltpu.HBM)
    dma = pltpu.SemaphoreType.DMA
    result = pl.pallas_call(
        functools.partial(fused, wins, chunks),
        out_shape=pltpu.VMEM((here, width), bf16),
        in_specs=[in_hbm] * 9,
        out_specs=pl.BlockSpec(memory_space=pltpu.VMEM),
        scratch_shapes=[
            pltpu.SMEM((1,), jnp.int32),
            pltpu.SMEM((1, 2), jnp.int32),
            pltpu.SMEM((1, 1), jnp.float32),
            pltpu.VMEM((here, width), bf16),
            pltpu.VMEM((here, width), bf16),
            pltpu.VMEM((3, steps, width), jnp.float32),
            pltpu.VMEM((3 * LANES, width), bf16),
            pltpu.VMEM((width, 3 * LANES), bf16),
            pltpu.VMEM((seq * (LANES * 3 // 4), width), bf16),
            pltpu.VMEM((EARLY, here, width), bf16),
            pltpu.VMEM((2, PIECES, (seq - EARLY) // 2, unit, width), bf16),
            pltpu.VMEM((2, seq * half, LANES), bf16),
            pltpu.VMEM((seq * here, LANES), bf16),
            pltpu.VMEM((seq * here, LANES), bf16),
            pltpu.VMEM((2, seq, half, LANES), bf16),
            pltpu.VMEM((2, seq, half, LANES), bf16),
            pltpu.VMEM((2, chunks, half, span), bf16),
            pltpu.VMEM((2, chunks, half, span), bf16),
            pltpu.VMEM((2, chunks, half, span), bf16),
            dma((7,)),
            dma((7,)),
            dma((2,)),
            dma((EARLY // 2 - 1, PIECES)),
            dma((EARLY // 2,)),
            dma((PIECES + 1,)),
            dma((PIECES + 1,)),
            dma((2,)),
            dma((2, chunks)),
            dma((1,)),
        ],
        compiler_params=pltpu.CompilerParams(
            collective_id=0, has_side_effects=True, vmem_limit_bytes=56 * 1024 * 1024
        ),
    )(
        latents.reshape(here, width),
        timesteps,
        offsets,
        qkv_weight[0, :, 0, :].T,
        logit_scale,
        out_weight[0],
        mod_shift[0],
        mod_scale[0],
        mod_gate[0],
    )
    return result.reshape(1, row_count, col_count, width)


def solution(mesh):
    in_specs = (
        P("segment", "seq", "win", None),
        P("segment"),
        P("segment", None),
        P("segment", None, "seq", None),
        P("segment", "seq"),
        P("segment", None, None),
        P("segment", None, None),
        P("segment", None, None),
        P("segment", None, None),
    )
    out_specs = P("segment", "seq", "win", None)
    return jax.shard_map(shards, mesh=mesh, in_specs=in_specs, out_specs=out_specs, check_vma=False)
```
